512 devices in a mesh: uly: 8 (over y, core), blk: 64 (over x, z).
Axes of the slice: x: 4, y: 4, z: 16, core: 2. Of those that a mesh axis runs over, the one named last changes fastest.
Arguments:
- query_inputs: bfloat16 [65536, 2048], P(('blk', 'uly')), may hold values from -6 to 6
- key_inputs: bfloat16 [65536, 1024], P(('blk', 'uly')), may hold values from -6 to 6
- value_inputs: bfloat16 [65536, 1024], P(('blk', 'uly')), may hold values from -6 to 6
- forward_out: bfloat16 [65536, 2048], P(('blk', 'uly')), may hold values from -6 to 6
- output_gradient: bfloat16 [65536, 2048], P(('blk', 'uly')), may hold values from -4 to 4
- lse_parts: float32 [65536, 16, 2], P(('blk', 'uly')), may hold values from 3 to 247
- segment_ids: int32 [65536], P(('blk', 'uly')), may hold values from 0 to 127, never falling along the last dimension, each value on 1 to 2048 neighbouring positions
Outputs:
- query_grad: bfloat16 [65536, 2048], P(('blk', 'uly'))
- key_grad: bfloat16 [65536, 1024], P(('blk', 'uly'))
- value_grad: bfloat16 [65536, 1024], P(('blk', 'uly'))
The draws below stay inside these ranges and needn't reach their ends.
Inputs may be any that keep to these rules, and one draw needn't show every extreme that they name: `segment_ids`: never falls along the sequence; every document holds 1 to 2048 tokens, and some document exactly 2048.
All inputs are finite; a program needn't handle non-finite values.
Results may differ from the reference program's by a relative error of at most 0.0051.
Values may be sent and summed in bfloat16 or wider, within the bound.
No kernel may reach another device: no remote copies, remote signals or barrier semaphores. Data moves between devices by JAX's collectives and lax.ppermute only.
A program may use at most 128 MiB of HBM per device.

```python
import math
import jax
import jax.numpy as jnp
import numpy as np
from jax import lax

HEAD_SIZE = 128
QUERY_HEADS = 16
KEY_VALUE_HEADS = 8
QBLOCK = 512
SEQUENCE_TOKENS = 65536
DOCUMENT_LIMIT = 2048
SEGS = 128


def draw_lse_parts(key, part):
    first_key = jax.random.fold_in(key, 0)
    shape_all = (SEQUENCE_TOKENS, QUERY_HEADS, 2)
    return jnp.clip(5.0 + 0.8 * jax.random.normal(first_key, shape_all, jnp.float32), 3.0, 7.0)


def shard_levels(key, dims, cuts, least, top_value):
    def one(dim, shards_of):
        draws = jax.random.uniform(jax.random.fold_in(jax.random.fold_in(key, 6), dim), (shards_of,), jnp.float32, least / len(cuts), top_value / len(cuts))
        return jnp.repeat(jnp.exp(draws), dims[dim] // shards_of).reshape((-1,) + (1,) * (len(dims) - dim - 1))

    loudness = one(*cuts[0])
    for cut in cuts[1:]:
        loudness = loudness * one(*cut)
    return loudness


def split_up(count, total, most, slope):
    loads = [(1 << 20) // math.isqrt(grade ** slope) + 1 for grade in range(2, count + 1)]
    rest, counts = total - most - (count - 1), [1] * (count - 1)
    while rest > 0:
        candidates = [i for i in range(count - 1) if counts[i] < most]
        pool, budget = sum([loads[i] for i in candidates]), rest
        for i in candidates:
            extra = min(most - counts[i], max(1, budget * loads[i] // pool), rest)
            counts[i] = counts[i] + extra
            rest = rest - extra
    return np.array([most] + counts)


def ragged_sizes(rng, number_of, total, bound, slope):
    if number_of == 2:
        one = jax.random.randint(rng, (), max(1, total - bound), min(bound, total - 1) + 1)
        return jnp.stack([one, total - one])
    sizes = jnp.asarray(split_up(number_of, total, bound, slope), jnp.int32)
    pairs = (number_of - 1) // 2
    donor, taker = sizes[1:1 + 2 * pairs:2], sizes[2:2 + 2 * pairs:2]
    room = jnp.minimum(donor - 1, bound - taker)
    passed = jax.random.randint(jax.random.fold_in(rng, 1), (pairs,), 0, 1 << 20) % (room + 1)
    sizes = sizes.at[1:1 + 2 * pairs:2].set(donor - passed).at[2:2 + 2 * pairs:2].set(taker + passed)
    return sizes[jax.random.permutation(jax.random.fold_in(rng, 2), number_of)]


def scatter_about(rng, extent, deviation, limit, cuts=(), kind=jnp.bfloat16):
    array = jax.random.normal(rng, extent, jnp.float32) * deviation
    if len(cuts) > 0:
        array = shard_levels(rng, extent, cuts, -0.22, 0.18) * array
    return jnp.clip(array, min=-limit, max=limit).astype(kind)


def setup_inputs(seed: int = 0) -> dict:
    keys = jax.random.split(jax.random.key(seed), 8)
    return {
        "query_inputs": scatter_about(keys[0], (SEQUENCE_TOKENS, QUERY_HEADS * HEAD_SIZE), 1.0, 6.0, ((0, 512),)),
        "key_inputs": scatter_about(keys[1], (SEQUENCE_TOKENS, KEY_VALUE_HEADS * HEAD_SIZE), 1.0, 6.0, ((0, 512),)),
        "value_inputs": scatter_about(keys[2], (SEQUENCE_TOKENS, KEY_VALUE_HEADS * HEAD_SIZE), 1.0, 6.0, ((0, 512),)),
        "forward_out": scatter_about(keys[3], (SEQUENCE_TOKENS, QUERY_HEADS * HEAD_SIZE), 0.5, 6.0, ((0, 512),)),
        "output_gradient": scatter_about(keys[4], (SEQUENCE_TOKENS, QUERY_HEADS * HEAD_SIZE), 0.25, 4.0, ((0, 512),)),
        "lse_parts": draw_lse_parts(jax.random.fold_in(keys[7], 71), 0),
        "segment_ids": jnp.searchsorted(jnp.cumsum(ragged_sizes(keys[6], SEGS, SEQUENCE_TOKENS, DOCUMENT_LIMIT, 2)), jnp.arange(SEQUENCE_TOKENS), side="right").astype(jnp.int32),
    }


def merge_parts(partials):
    highest = lax.optimization_barrier(jnp.max(partials, axis=-1))
    return highest + jnp.log(lax.optimization_barrier(jnp.sum(jnp.exp(partials - highest[..., None]), axis=-1)))

def round_trip(values_in):
    rounded = lax.optimization_barrier(values_in.astype(jnp.bfloat16))
    return rounded.astype(jnp.float32)

def reference(query_inputs, key_inputs, value_inputs, forward_out, output_gradient, lse_parts, segment_ids):
    token_count = query_inputs.shape[0]
    group_width = QUERY_HEADS // KEY_VALUE_HEADS
    score_scale = 1.0 / math.sqrt(HEAD_SIZE)
    rows_per_block = min(QBLOCK, token_count)
    lookback_span = DOCUMENT_LIMIT + rows_per_block
    logsumexp_rows = merge_parts(lse_parts)
    products = output_gradient.astype(jnp.float32) * forward_out.astype(jnp.float32)
    row_deltas = lax.optimization_barrier(jnp.sum(products.reshape(token_count, QUERY_HEADS, HEAD_SIZE), axis=-1))
    key_with_padding = jnp.pad(key_inputs, ((DOCUMENT_LIMIT, 0), (0, 0)))
    value_with_padding = jnp.pad(value_inputs, ((DOCUMENT_LIMIT, 0), (0, 0)))
    ids_padded = jnp.concatenate([jnp.full((DOCUMENT_LIMIT,), -1, jnp.int32), segment_ids.astype(jnp.int32)])

    def block_step(carried, block_index):
        key_gradient_running, value_gradient_running = carried
        leading_row = (block_index * rows_per_block).astype(jnp.int32)
        query_quad = lax.dynamic_slice_in_dim(query_inputs, leading_row, rows_per_block, 0).astype(jnp.float32).reshape(rows_per_block, KEY_VALUE_HEADS, group_width, HEAD_SIZE)
        gradient_quad = lax.dynamic_slice_in_dim(output_gradient, leading_row, rows_per_block, 0).astype(jnp.float32).reshape(rows_per_block, KEY_VALUE_HEADS, group_width, HEAD_SIZE)
        logsumexp_cube = lax.dynamic_slice_in_dim(logsumexp_rows, leading_row, rows_per_block, 0).reshape(rows_per_block, KEY_VALUE_HEADS, group_width).transpose(1, 2, 0)[..., None]
        delta_cube = lax.dynamic_slice_in_dim(row_deltas, leading_row, rows_per_block, 0).reshape(rows_per_block, KEY_VALUE_HEADS, group_width).transpose(1, 2, 0)[..., None]
        key_cube = lax.dynamic_slice_in_dim(key_with_padding, leading_row, lookback_span, 0).astype(jnp.float32).reshape(lookback_span, KEY_VALUE_HEADS, HEAD_SIZE)
        value_cube = lax.dynamic_slice_in_dim(value_with_padding, leading_row, lookback_span, 0).astype(jnp.float32).reshape(lookback_span, KEY_VALUE_HEADS, HEAD_SIZE)
        query_ids = lax.dynamic_slice_in_dim(segment_ids.astype(jnp.int32), leading_row, rows_per_block, 0)
        key_ids = lax.dynamic_slice_in_dim(ids_padded, leading_row, lookback_span, 0)
        query_pos = leading_row + DOCUMENT_LIMIT + jnp.arange(rows_per_block, dtype=jnp.int32)
        key_pos = leading_row + jnp.arange(lookback_span, dtype=jnp.int32)
        allowed = (key_pos[None, :] <= query_pos[:, None]) & (key_ids[None, :] == query_ids[:, None])
        scores = jnp.einsum('mhgd,nhd->hgmn', query_quad, key_cube) * score_scale
        weights = jnp.where(allowed, jnp.exp(scores - logsumexp_cube), 0.0)
        value_portion = jnp.einsum('hgmn,mhgd->nhd', round_trip(weights), gradient_quad)
        prob_grad = jnp.einsum('mhgd,nhd->hgmn', gradient_quad, value_cube)
        score_grad = round_trip(weights * (prob_grad - delta_cube))
        query_part = jnp.einsum('hgmn,nhd->mhgd', score_grad, key_cube) * score_scale
        key_portion = jnp.einsum('hgmn,mhgd->nhd', score_grad, query_quad) * score_scale
        key_window_rows = lax.dynamic_slice_in_dim(key_gradient_running, leading_row, lookback_span, 0) + key_portion.reshape(lookback_span, KEY_VALUE_HEADS * HEAD_SIZE)
        value_window_rows = lax.dynamic_slice_in_dim(value_gradient_running, leading_row, lookback_span, 0) + value_portion.reshape(lookback_span, KEY_VALUE_HEADS * HEAD_SIZE)
        key_gradient_running = lax.dynamic_update_slice_in_dim(key_gradient_running, key_window_rows, leading_row, 0)
        value_gradient_running = lax.dynamic_update_slice_in_dim(value_gradient_running, value_window_rows, leading_row, 0)
        return ((key_gradient_running, value_gradient_running), query_part.reshape(rows_per_block, QUERY_HEADS * HEAD_SIZE).astype(jnp.bfloat16))
    initial_running = (jnp.zeros((token_count + DOCUMENT_LIMIT, KEY_VALUE_HEADS * HEAD_SIZE), jnp.float32), jnp.zeros((token_count + DOCUMENT_LIMIT, KEY_VALUE_HEADS * HEAD_SIZE), jnp.float32))
    final_acc, query_blocks = lax.scan(block_step, initial_running, jnp.arange(token_count // rows_per_block, dtype=jnp.int32))
    query_grad = query_blocks.reshape(token_count, QUERY_HEADS * HEAD_SIZE)
    key_grad = final_acc[0][DOCUMENT_LIMIT:].astype(jnp.bfloat16)
    value_grad = final_acc[1][DOCUMENT_LIMIT:].astype(jnp.bfloat16)
    return (query_grad, key_grad, value_grad)
```

```python
import functools
import math

import jax
import jax.numpy as jnp
from jax import lax
from jax.experimental import pallas as pl
from jax.experimental.pallas import tpu as pltpu
from jax.sharding import Mesh
from jax.sharding import PartitionSpec as P

D = 128
T = 128
U = 8
KB = 256
QP = 2
STAT = 16
KROWS = 2 * T + STAT
QROWS = 4 * T + STAT
SCALE = 1.0 / math.sqrt(D)
LOG2E = 1.4426950408889634
ULY = ("uly_0", "uly_1")
BLK_ULY = ("blk", "uly_0", "uly_1")
F32 = jnp.float32
BF16 = jnp.bfloat16
VM = pl.BlockSpec(memory_space=pltpu.VMEM)


def dot(a, b, ca, cb):
    return lax.dot_general(a, b, (((ca,), (cb,)), ((), ())), preferred_element_type=F32)


def pack_kv_kernel(k_ref, v_ref, id_ref, out_ref):
    ids = jnp.broadcast_to(id_ref[...].astype(F32), (STAT, T)).astype(BF16)
    for j in range(U):
        out_ref[j, 0:T, :] = k_ref[:, j * D : (j + 1) * D]
        out_ref[j, T : 2 * T, :] = v_ref[:, j * D : (j + 1) * D]
        out_ref[j, 2 * T :, :] = ids


def three(x):
    hi = x.astype(BF16).astype(F32)
    rest = x - hi
    mid = rest.astype(BF16).astype(F32)
    return hi, mid, (rest - mid).astype(BF16).astype(F32)


def pack_q_kernel(q_ref, g_ref, o_ref, lse_ref, out_ref):
    first, second = lse_ref[:, 0, :], lse_ref[:, 1, :]
    top = jnp.maximum(first, second)
    lse = top + jnp.log(jnp.exp(first - top) + jnp.exp(second - top))
    lane = lax.broadcasted_iota(jnp.int32, (T, D), 1)
    deltas = jnp.zeros((T, D), F32)
    for h in range(2 * U):
        cols = slice(h * D, (h + 1) * D)
        prod = g_ref[:, cols].astype(F32) * o_ref[:, cols].astype(F32)
        deltas = jnp.where(lane == h, jnp.sum(prod, axis=1, keepdims=True), deltas)
        j, g = divmod(h, 2)
        out_ref[j, g * T : (g + 1) * T, :] = q_ref[:, cols]
        out_ref[j, (2 + g) * T : (3 + g) * T, :] = g_ref[:, cols]
    parts = three(lse) + three(deltas.T)
    for j in range(U):
        rows = [p[2 * j : 2 * j + 2, :] for p in parts] + [jnp.zeros((4, T), F32)]
        out_ref[j, 4 * T :, :] = jnp.concatenate(rows, axis=0).astype(BF16)


def fill_rows(q_ref, own_ref, lse_s, del_s, qid_s):
    for u in range(U):
        st = q_ref[u, 4 * T :, :].astype(F32)
        two = st[0:2] + st[2:4] + st[4:6]
        dlt = st[6:8] + st[8:10] + st[10:12]
        ids = own_ref[u, 2 * T : 2 * T + 1, :].astype(F32)
        for g in range(2):
            lse_s[u, 0:1, g * T : (g + 1) * T] = two[g : g + 1] * LOG2E
            del_s[u, 0:1, g * T : (g + 1) * T] = dlt[g : g + 1]
        qid_s[u, 0:1, :] = ids


def fill_keys(kv_refs, k_s, v_s, kid_s):
    pick = (lax.broadcasted_iota(jnp.int32, (STAT, D), 0) == 0).astype(F32).astype(BF16)
    for w, ref in enumerate(kv_refs):
        for u in range(U):
            b, r = divmod(w * U + u, KB // T)
            rows = slice(r * T, (r + 1) * T)
            k_s[b, rows, :] = ref[u, 0:T, :]
            v_s[b, rows, :] = ref[u, T : 2 * T, :]
            kid_s[b, rows, :] = dot(ref[u, 2 * T :, :], pick, 0, 0)


def matching(kv_ref, qid, upto):
    total = jnp.zeros((1, T), F32)
    for u in range(upto):
        ids = kv_ref[u, 2 * T : 2 * T + 1, :].astype(F32)
        total = total + jnp.where(ids == qid, 1.0, 0.0)
    return total


def tile(q_ref, k_s, v_s, kid_s, lse_s, del_s, qid_s, dq_s, dkv_ref, qb, kb, causal, key_base):
    k, v = k_s[kb], v_s[kb]
    us = [qb * QP + i for i in range(QP)]
    q = jnp.concatenate([q_ref[u, 0 : 2 * T, :] for u in us], axis=0)
    g = jnp.concatenate([q_ref[u, 2 * T : 4 * T, :] for u in us], axis=0)
    st = dot(k, q, 1, 1)
    dpt = dot(v, g, 1, 1)
    kid = kid_s[kb]
    if causal:
        kpos = lax.broadcasted_iota(jnp.int32, (KB, T), 0) + (kb * KB - key_base)
        qpos = lax.broadcasted_iota(jnp.int32, (KB, T), 1)
    ps, dss = [], []
    for i, u in enumerate(us):
        okay = kid == qid_s[u, 0:1, :]
        if causal:
            okay = okay & (kpos <= qpos + u * T)
        for h in range(2):
            c = slice((2 * i + h) * T, (2 * i + h + 1) * T)
            r = slice(h * T, (h + 1) * T)
            p = jnp.where(okay, jnp.exp2(st[:, c] * (SCALE * LOG2E) - lse_s[u, 0:1, r]), 0.0)
            ps.append(p.astype(BF16))
            dss.append((p * (dpt[:, c] - del_s[u, 0:1, r])).astype(BF16))
    p = jnp.concatenate(ps, axis=1)
    ds = jnp.concatenate(dss, axis=1)
    dv = dot(p, g, 1, 0)
    dk = dot(ds, q, 1, 0)
    dq = dot(k, ds, 0, 0)
    for r in range(KB // T):
        piece = kb * (KB // T) + r
        rows = slice(r * T, (r + 1) * T)
        dkv_ref[piece, 0:T, :] += dk[rows]
        dkv_ref[piece, T : 2 * T, :] += dv[rows]
    for i, u in enumerate(us):
        dq_s[u] += dq[:, i * 2 * T : (i + 1) * 2 * T]


def near_kernel(q_ref, own_ref, prev_ref, dq_ref, dkv_ref, k_s, v_s, kid_s, lse_s, del_s, qid_s):
    fill_rows(q_ref, own_ref, lse_s, del_s, qid_s)
    fill_keys((prev_ref, own_ref), k_s, v_s, kid_s)
    dq_ref[...] = jnp.zeros_like(dq_ref)
    dkv_ref[...] = jnp.zeros_like(dkv_ref)
    for qb in range(U // QP):
        head = qid_s[qb * QP, 0:1, 0:1]
        live = jnp.sum(matching(prev_ref, head, U) + matching(own_ref, head, qb * QP))
        start = U * T + qb * QP * T - live.astype(jnp.int32)

        @pl.loop(start // KB, (U * T + (qb + 1) * QP * T) // KB)
        def _(kb, qb=qb):
            tile(q_ref, k_s, v_s, kid_s, lse_s, del_s, qid_s, dq_ref, dkv_ref, qb, kb, True, U * T)


def far_kernel(
    q_ref, own_ref, far_ref, dqin_ref, dq_ref, dkv_ref, acc_s, dkv_s, k_s, v_s, kid_s, lse_s, del_s, qid_s
):
    fill_rows(q_ref, own_ref, lse_s, del_s, qid_s)
    fill_keys((far_ref,), k_s, v_s, kid_s)
    acc_s[...] = dqin_ref[...]
    dkv_s[...] = jnp.zeros_like(dkv_s)
    for qb in range(U // QP):
        head = qid_s[qb * QP, 0:1, 0:1]
        live = jnp.sum(matching(far_ref, head, U)).astype(jnp.int32)

        @pl.loop((U * T - live) // KB, U * T // KB)
        def _(kb, qb=qb):
            tile(q_ref, k_s, v_s, kid_s, lse_s, del_s, qid_s, acc_s, dkv_s, qb, kb, False, 0)

    for u in range(U):
        dkv_ref[u, 0:T, :] = (dkv_s[u, 0:T, :] * SCALE).astype(BF16)
        dkv_ref[u, T : 2 * T, :] = dkv_s[u, T : 2 * T, :].astype(BF16)
        for h in range(2):
            c = slice(h * T, (h + 1) * T)
            dq_ref[u, c, :] = (acc_s[u, :, c].T * SCALE).astype(BF16)


def add_kernel(base, part_ref, more_ref, out_ref):
    for u in range(U):
        dk = part_ref[base + u, 0:T, :] * SCALE
        out_ref[u, 0:T, :] = (dk + more_ref[u, 0:T, :].astype(F32)).astype(BF16)
        dv = part_ref[base + u, T : 2 * T, :]
        out_ref[u, T : 2 * T, :] = (dv + more_ref[u, T : 2 * T, :].astype(F32)).astype(BF16)


def unpack_q_kernel(in_ref, out_ref):
    for h in range(2 * U):
        j, g = divmod(h, 2)
        out_ref[:, h * D : (h + 1) * D] = in_ref[j, g * T : (g + 1) * T, :]


def unpack_kv_kernel(in_ref, k_ref, v_ref):
    for j in range(U):
        k_ref[:, j * D : (j + 1) * D] = in_ref[j, 0:T, :]
        v_ref[:, j * D : (j + 1) * D] = in_ref[j, T : 2 * T, :]


def call(kernel, outs, scratch=(), flops=0, name=None):
    many = isinstance(outs, tuple)
    return pl.pallas_call(
        kernel,
        out_shape=outs,
        out_specs=(VM,) * len(outs) if many else VM,
        scratch_shapes=scratch,
        cost_estimate=pl.CostEstimate(flops=flops, bytes_accessed=1 << 20, transcendentals=0),
        name=name,
    )


def key_scratch(windows):
    blocks = windows * U * T // KB
    return [
        pltpu.VMEM((blocks, KB, D), BF16),
        pltpu.VMEM((blocks, KB, D), BF16),
        pltpu.VMEM((blocks, KB, D), F32),
        pltpu.VMEM((U, 8, 2 * T), F32),
        pltpu.VMEM((U, 8, 2 * T), F32),
        pltpu.VMEM((U, 8, T), F32),
    ]


def shape(*dims, dtype=BF16):
    return jax.ShapeDtypeStruct(dims, dtype)


def exchanged(message):
    return lax.all_to_all(message, ULY, 0, 0, tiled=True)


def moved(block, distance):
    count = lax.axis_size("blk")
    return lax.ppermute(block, "blk", [(i, (i + distance) % count) for i in range(count)])


def per_device(query, key, value, forward_out, out_grad, lse_parts, ids):
    kv_msg = call(pack_kv_kernel, shape(U, KROWS, D), flops=1 << 20, name="pack_kv")(
        key, value, ids.reshape(1, T)
    )
    own = exchanged(kv_msg)
    q_msg = call(pack_q_kernel, shape(U, QROWS, D), flops=1 << 20, name="pack_q")(
        query, out_grad, forward_out, lse_parts.transpose(1, 2, 0)
    )
    prev = moved(own, 1)
    rows = exchanged(q_msg)
    far = moved(prev, 1)
    dq, dkv = call(
        near_kernel,
        (shape(U, D, 2 * T, dtype=F32), shape(2 * U, 2 * T, D, dtype=F32)),
        key_scratch(2),
        flops=8 << 30,
        name="near",
    )(rows, own, prev)
    dq_msg, far_msg = call(
        far_kernel,
        (shape(U, 2 * T, D), shape(U, 2 * T, D)),
        [pltpu.VMEM((U, D, 2 * T), F32), pltpu.VMEM((U, 2 * T, D), F32)] + key_scratch(1),
        flops=2 << 30,
        name="far",
    )(rows, own, far, dq)
    back = moved(far_msg, -1)
    dq_rows = exchanged(dq_msg)
    prev_msg = call(functools.partial(add_kernel, 0), shape(U, 2 * T, D), flops=1 << 20, name="add_prev")(
        dkv, back
    )
    back = moved(prev_msg, -1)
    query_grad = call(unpack_q_kernel, shape(T, 2 * U * D), flops=1 << 20, name="unpack_q")(dq_rows)
    own_msg = call(functools.partial(add_kernel, U), shape(U, 2 * T, D), flops=1 << 20, name="add_own")(
        dkv, back
    )
    key_grad, value_grad = call(
        unpack_kv_kernel, (shape(T, U * D), shape(T, U * D)), flops=1 << 20, name="unpack_kv"
    )(exchanged(own_msg))
    return query_grad, key_grad, value_grad


def solution(mesh):
    torus = Mesh(mesh.devices.reshape(4, 2, mesh.shape["blk"]), ("uly_0", "uly_1", "blk"))
    flat, cube, line = P(BLK_ULY, None), P(BLK_ULY, None, None), P(BLK_ULY)
    return jax.shard_map(
        per_device,
        mesh=torus,
        in_specs=(flat, flat, flat, flat, flat, cube, line),
        out_specs=(flat, flat, flat),
        check_vma=False,
    )
```

```python
import math

import jax
import jax.numpy as jnp
from jax import lax
from jax.experimental import pallas as pl
from jax.experimental.pallas import tpu as pltpu
from jax.sharding import Mesh
from jax.sharding import PartitionSpec as P


D = 128
T = 128
U = 8
KB = 256
QP = 2
STAT = 16
KROWS = 2 * T + STAT
QROWS = 4 * T + STAT
SCALE = 1.0 / math.sqrt(D)
LOG2E = 1.4426950408889634
ULY = ("uly_0", "uly_1")
BLK_ULY = ("blk", "uly_0", "uly_1")
F32 = jnp.float32
BF16 = jnp.bfloat16
VM = pl.BlockSpec(memory_space=pltpu.VMEM)


def dot(a, b, ca, cb):
    return lax.dot_general(a, b, (((ca,), (cb,)), ((), ())), preferred_element_type=F32)


def pack_kv_kernel(k_ref, v_ref, id_ref, out_ref):
    ids = jnp.broadcast_to(id_ref[...].astype(F32), (STAT, T)).astype(BF16)
    for j in range(U):
        out_ref[j, 0:T, :] = k_ref[:, j * D : (j + 1) * D]
        out_ref[j, T : 2 * T, :] = v_ref[:, j * D : (j + 1) * D]
        out_ref[j, 2 * T :, :] = ids


def three(x):
    hi = x.astype(BF16).astype(F32)
    rest = x - hi
    mid = rest.astype(BF16).astype(F32)
    return hi, mid, (rest - mid).astype(BF16).astype(F32)


def pack_all_kernel(q_ref, g_ref, o_ref, lse_ref, id_ref, kv_ref, out_ref):
    first, second = lse_ref[:, 0, :], lse_ref[:, 1, :]
    top = jnp.maximum(first, second)
    lse = top + jnp.log(jnp.exp(first - top) + jnp.exp(second - top))
    lane = lax.broadcasted_iota(jnp.int32, (T, D), 1)
    deltas = jnp.zeros((T, D), F32)
    for h in range(2 * U):
        cols = slice(h * D, (h + 1) * D)
        prod = g_ref[:, cols].astype(F32) * o_ref[:, cols].astype(F32)
        deltas = jnp.where(lane == h, jnp.sum(prod, axis=1, keepdims=True), deltas)
        j, g = divmod(h, 2)
        out_ref[j, g * T : (g + 1) * T, :] = q_ref[:, cols]
        out_ref[j, (2 + g) * T : (3 + g) * T, :] = g_ref[:, cols]
    parts = three(lse) + three(deltas.T)
    ids = jnp.broadcast_to(id_ref[...].astype(F32), (4, T))
    for j in range(U):
        rows = [p[2 * j : 2 * j + 2, :] for p in parts] + [ids]
        out_ref[j, 4 * T : QROWS, :] = jnp.concatenate(rows, axis=0).astype(BF16)
        out_ref[j, QROWS:, :] = kv_ref[j]


def fill_rows(q_ref, lse_s, del_s, qid_s):
    for u in range(U):
        st = q_ref[u, 4 * T : QROWS, :].astype(F32)
        two = st[0:2] + st[2:4] + st[4:6]
        dlt = st[6:8] + st[8:10] + st[10:12]
        for g in range(2):
            lse_s[u, 0:1, g * T : (g + 1) * T] = two[g : g + 1] * LOG2E
            del_s[u, 0:1, g * T : (g + 1) * T] = dlt[g : g + 1]
        qid_s[u, 0:1, :] = st[12:13]


def fill_keys(kv_ref, first, k_s, v_s, kid_s):
    pick = (lax.broadcasted_iota(jnp.int32, (STAT, D), 0) == 0).astype(F32).astype(BF16)
    for u in range(U):
        b, r = divmod(u, KB // T)
        rows = slice(r * T, (r + 1) * T)
        k_s[b, rows, :] = kv_ref[u, first : first + T, :]
        v_s[b, rows, :] = kv_ref[u, first + T : first + 2 * T, :]
        kid_s[b, rows, :] = dot(kv_ref[u, first + 2 * T : first + KROWS, :], pick, 0, 0)


def matching(kv_ref, first, qid, upto):
    total = jnp.zeros((1, T), F32)
    for u in range(upto):
        ids = kv_ref[u, first + 2 * T : first + 2 * T + 1, :].astype(F32)
        total = total + jnp.where(ids == qid, 1.0, 0.0)
    return jnp.sum(total).astype(jnp.int32)


def tile(q_ref, k_s, v_s, kid_s, lse_s, del_s, qid_s, dq_s, dkv_ref, qb, kb, causal):
    k, v = k_s[kb], v_s[kb]
    us = [qb * QP + i for i in range(QP)]
    q = jnp.concatenate([q_ref[u, 0 : 2 * T, :] for u in us], axis=0)
    g = jnp.concatenate([q_ref[u, 2 * T : 4 * T, :] for u in us], axis=0)
    st = dot(k, q, 1, 1)
    dpt = dot(v, g, 1, 1)
    kid = kid_s[kb]
    if causal:
        kpos = lax.broadcasted_iota(jnp.int32, (KB, T), 0) + kb * KB
        qpos = lax.broadcasted_iota(jnp.int32, (KB, T), 1)
    ps, dss = [], []
    for i, u in enumerate(us):
        okay = kid == qid_s[u, 0:1, :]
        if causal:
            okay = okay & (kpos <= qpos + u * T)
        for h in range(2):
            c = slice((2 * i + h) * T, (2 * i + h + 1) * T)
            r = slice(h * T, (h + 1) * T)
            p = jnp.where(okay, jnp.exp2(st[:, c] * (SCALE * LOG2E) - lse_s[u, 0:1, r]), 0.0)
            ps.append(p.astype(BF16))
            dss.append((p * (dpt[:, c] - del_s[u, 0:1, r])).astype(BF16))
    p = jnp.concatenate(ps, axis=1)
    ds = jnp.concatenate(dss, axis=1)
    dv = dot(p, g, 1, 0)
    dk = dot(ds, q, 1, 0)
    dq = dot(k, ds, 0, 0)
    for r in range(KB // T):
        piece = kb * (KB // T) + r
        rows = slice(r * T, (r + 1) * T)
        dkv_ref[piece, 0:T, :] += dk[rows]
        dkv_ref[piece, T : 2 * T, :] += dv[rows]
    for i, u in enumerate(us):
        dq_s[u] += dq[:, i * 2 * T : (i + 1) * 2 * T]


def turned(acc, u, h):
    return acc[u, :, h * T : (h + 1) * T].T * SCALE


def start_sums(dq_s, dkv_s):
    dq_s[...] = jnp.zeros_like(dq_s)
    dkv_s[...] = jnp.zeros_like(dkv_s)


def walk(q_ref, kv_ref, first, causal, dq_s, dkv_s, k_s, v_s, kid_s, lse_s, del_s, qid_s):
    fill_rows(q_ref, lse_s, del_s, qid_s)
    fill_keys(kv_ref, first, k_s, v_s, kid_s)
    for qb in range(U // QP):
        head = qid_s[qb * QP, 0:1, 0:1]
        before = qb * QP if causal else U
        upto = (qb + 1) * QP if causal else U
        live = matching(kv_ref, first, head, before)

        @pl.loop((before * T - live) // KB, upto * T // KB)
        def _(kb, qb=qb):
            tile(q_ref, k_s, v_s, kid_s, lse_s, del_s, qid_s, dq_s, dkv_s, qb, kb, causal)


def own_kernel(all_ref, dq_ref, dkv_ref, *scratch):
    start_sums(dq_ref, dkv_ref)
    walk(all_ref, all_ref, QROWS, True, dq_ref, dkv_ref, *scratch)
    for u in range(U):
        dkv_ref[u, 0:T, :] = dkv_ref[u, 0:T, :] * SCALE


def prev_kernel(all_ref, prev_ref, sum_ref, dq_ref, dkv_ref, dq_s, *scratch):
    dq_s[...] = sum_ref[...]
    dkv_ref[...] = jnp.zeros_like(dkv_ref)
    walk(all_ref, prev_ref, 0, False, dq_s, dkv_ref, *scratch)
    for u in range(U):
        for h in range(2):
            dq_ref[u, h * T : (h + 1) * T, :] = turned(dq_s, u, h)


def far_kernel(q_ref, prev_ref, sum_ref, dq_ref, dkv_ref, dq_s, dkv_s, *scratch):
    dq_s[...] = jnp.zeros_like(dq_s)
    dkv_s[...] = sum_ref[...]
    walk(q_ref, prev_ref, 0, False, dq_s, dkv_s, *scratch)
    for u in range(U):
        dkv_ref[u, 0:T, :] = (dkv_s[u, 0:T, :] * SCALE).astype(BF16)
        dkv_ref[u, T : 2 * T, :] = dkv_s[u, T : 2 * T, :].astype(BF16)
        for h in range(2):
            dq_ref[u, h * T : (h + 1) * T, :] = turned(dq_s, u, h).astype(BF16)


def total_kernel(dq_ref, more_q_ref, dkv_ref, more_kv_ref, out_ref):
    for u in range(U):
        out_ref[u, 0 : 2 * T, :] = (dq_ref[u] + more_q_ref[u].astype(F32)).astype(BF16)
        out_ref[u, 2 * T :, :] = (dkv_ref[u] + more_kv_ref[u].astype(F32)).astype(BF16)


def unpack_kernel(in_ref, q_ref, k_ref, v_ref):
    for j in range(U):
        for g in range(2):
            h = 2 * j + g
            q_ref[:, h * D : (h + 1) * D] = in_ref[j, g * T : (g + 1) * T, :]
        k_ref[:, j * D : (j + 1) * D] = in_ref[j, 2 * T : 3 * T, :]
        v_ref[:, j * D : (j + 1) * D] = in_ref[j, 3 * T : 4 * T, :]


def call(kernel, outs, scratch=(), flops=0, limit=16):
    many = isinstance(outs, tuple)
    return pl.pallas_call(
        kernel,
        out_shape=outs,
        out_specs=(VM,) * len(outs) if many else VM,
        scratch_shapes=scratch,
        cost_estimate=pl.CostEstimate(flops=flops, bytes_accessed=1 << 20, transcendentals=0),
        compiler_params=pltpu.CompilerParams(vmem_limit_bytes=limit << 20),
    )


KEYS = (
    pltpu.VMEM((U * T // KB, KB, D), BF16),
    pltpu.VMEM((U * T // KB, KB, D), BF16),
    pltpu.VMEM((U * T // KB, KB, D), F32),
    pltpu.VMEM((U, 8, 2 * T), F32),
    pltpu.VMEM((U, 8, 2 * T), F32),
    pltpu.VMEM((U, 8, T), F32),
)
SUM_Q = pltpu.VMEM((U, D, 2 * T), F32)
SUM_KV = pltpu.VMEM((U, 2 * T, D), F32)


def shape(*dims, dtype=BF16):
    return jax.ShapeDtypeStruct(dims, dtype)


def exchanged(message):
    return lax.all_to_all(message, ULY, 0, 0, tiled=True)


def moved(block, distance):
    count = lax.axis_size("blk")
    return lax.ppermute(block, "blk", [(i, (i + distance) % count) for i in range(count)])


def stages(query, key, value, forward_out, out_grad, lse_parts, ids):
    ids = ids.reshape(1, T)
    kv_msg = call(pack_kv_kernel, shape(U, KROWS, D), flops=1 << 20, limit=56)(key, value, ids)
    prev_raw = moved(kv_msg, 1)
    message = call(pack_all_kernel, shape(U, QROWS + KROWS, D), flops=1 << 20, limit=56)(
        query, out_grad, forward_out, lse_parts.transpose(1, 2, 0), ids, kv_msg
    )
    rows = exchanged(message)
    later_rows = moved(rows[:, :QROWS], -1)
    prev = exchanged(prev_raw)
    tall, wide = shape(U, 2 * T, D, dtype=F32), shape(U, D, 2 * T, dtype=F32)
    dq, down = call(own_kernel, (wide, tall), KEYS, flops=4 << 30)(rows)
    dq, dprev = call(prev_kernel, (tall, tall), (SUM_Q,) + KEYS, flops=4 << 30)(rows, prev, dq)
    half = shape(U, 2 * T, D)
    dq_msg, dkv_msg = call(far_kernel, (half, half), (SUM_Q, SUM_KV) + KEYS, flops=1 << 30)(later_rows, prev, dprev)
    total = call(total_kernel, shape(U, 4 * T, D), flops=1 << 20)(dq, moved(dq_msg, 1), down, moved(dkv_msg, -1))
    return call(unpack_kernel, (shape(T, 2 * U * D), shape(T, U * D), shape(T, U * D)), flops=1 << 20)(exchanged(total))


def solution(mesh):
    torus = Mesh(mesh.devices.reshape(4, 2, mesh.shape["blk"]), ("uly_0", "uly_1", "blk"))
    flat, cube, line = P(BLK_ULY, None), P(BLK_ULY, None, None), P(BLK_ULY)
    return jax.shard_map(
        stages,
        mesh=torus,
        in_specs=(flat, flat, flat, flat, flat, cube, line),
        out_specs=(flat, flat, flat),
        check_vma=False,
    )
```

```python
import math

import jax
import jax.numpy as jnp
from jax import lax
from jax.experimental import pallas as pl
from jax.experimental.pallas import tpu as pltpu
from jax.sharding import Mesh
from jax.sharding import PartitionSpec as P


D = 128
T = 128
U = 8
KB = 256
QP = 2
STAT = 16
KROWS = 2 * T + STAT
QROWS = 4 * T + STAT
SCALE = 1.0 / math.sqrt(D)
LOG2E = 1.4426950408889634
ULY = ("uly_0", "uly_1")
BLK_ULY = ("blk", "uly_0", "uly_1")
F32 = jnp.float32
BF16 = jnp.bfloat16
VM = pl.BlockSpec(memory_space=pltpu.VMEM)


def dot(a, b, ca, cb):
    return lax.dot_general(a, b, (((ca,), (cb,)), ((), ())), preferred_element_type=F32)


def pack_kv_kernel(k_ref, v_ref, id_ref, out_ref):
    ids = jnp.broadcast_to(id_ref[...].astype(F32), (STAT, T)).astype(BF16)
    for j in range(U):
        out_ref[j, 0:T, :] = k_ref[:, j * D : (j + 1) * D]
        out_ref[j, T : 2 * T, :] = v_ref[:, j * D : (j + 1) * D]
        out_ref[j, 2 * T :, :] = ids


def three(x):
    hi = x.astype(BF16).astype(F32)
    rest = x - hi
    mid = rest.astype(BF16).astype(F32)
    return hi, mid, (rest - mid).astype(BF16).astype(F32)


def pack_q_kernel(q_ref, g_ref, o_ref, lse_ref, id_ref, out_ref):
    first, second = lse_ref[:, 0, :], lse_ref[:, 1, :]
    top = jnp.maximum(first, second)
    lse = top + jnp.log(jnp.exp(first - top) + jnp.exp(second - top))
    lane = lax.broadcasted_iota(jnp.int32, (T, D), 1)
    deltas = jnp.zeros((T, D), F32)
    for h in range(2 * U):
        cols = slice(h * D, (h + 1) * D)
        prod = g_ref[:, cols].astype(F32) * o_ref[:, cols].astype(F32)
        deltas = jnp.where(lane == h, jnp.sum(prod, axis=1, keepdims=True), deltas)
        j, g = divmod(h, 2)
        out_ref[j, g * T : (g + 1) * T, :] = q_ref[:, cols]
        out_ref[j, (2 + g) * T : (3 + g) * T, :] = g_ref[:, cols]
    parts = three(lse) + three(deltas.T)
    ids = jnp.broadcast_to(id_ref[...].astype(F32), (4, T))
    for j in range(U):
        rows = [p[2 * j : 2 * j + 2, :] for p in parts] + [ids]
        out_ref[j, 4 * T : QROWS, :] = jnp.concatenate(rows, axis=0).astype(BF16)


def fill_rows(q_ref, lse_s, del_s, qid_s):
    for u in range(U):
        st = q_ref[u, 4 * T : QROWS, :].astype(F32)
        two = st[0:2] + st[2:4] + st[4:6]
        dlt = st[6:8] + st[8:10] + st[10:12]
        for g in range(2):
            lse_s[u, 0:1, g * T : (g + 1) * T] = two[g : g + 1] * LOG2E
            del_s[u, 0:1, g * T : (g + 1) * T] = dlt[g : g + 1]
        qid_s[u, 0:1, :] = st[12:13]


def fill_keys(kv_ref, first, k_s, v_s, kid_s):
    pick = (lax.broadcasted_iota(jnp.int32, (STAT, D), 0) == 0).astype(F32).astype(BF16)
    for u in range(U):
        b, r = divmod(u, KB // T)
        rows = slice(r * T, (r + 1) * T)
        k_s[b, rows, :] = kv_ref[u, first : first + T, :]
        v_s[b, rows, :] = kv_ref[u, first + T : first + 2 * T, :]
        kid_s[b, rows, :] = dot(kv_ref[u, first + 2 * T : first + KROWS, :], pick, 0, 0)


def matching(kv_ref, first, qid, upto):
    total = jnp.zeros((1, T), F32)
    for u in range(upto):
        ids = kv_ref[u, first + 2 * T : first + 2 * T + 1, :].astype(F32)
        total = total + jnp.where(ids == qid, 1.0, 0.0)
    return jnp.sum(total).astype(jnp.int32)


def tile(q_ref, k_s, v_s, kid_s, lse_s, del_s, qid_s, dq_s, dkv_ref, qb, kb, causal):
    k, v = k_s[kb], v_s[kb]
    us = [qb * QP + i for i in range(QP)]
    q = jnp.concatenate([q_ref[u, 0 : 2 * T, :] for u in us], axis=0)
    g = jnp.concatenate([q_ref[u, 2 * T : 4 * T, :] for u in us], axis=0)
    st = dot(k, q, 1, 1)
    dpt = dot(v, g, 1, 1)
    kid = kid_s[kb]
    if causal:
        kpos = lax.broadcasted_iota(jnp.int32, (KB, T), 0) + kb * KB
        qpos = lax.broadcasted_iota(jnp.int32, (KB, T), 1)
    ps, dss = [], []
    for i, u in enumerate(us):
        okay = kid == qid_s[u, 0:1, :]
        if causal:
            okay = okay & (kpos <= qpos + u * T)
        for h in range(2):
            c = slice((2 * i + h) * T, (2 * i + h + 1) * T)
            r = slice(h * T, (h + 1) * T)
            p = jnp.where(okay, jnp.exp2(st[:, c] * (SCALE * LOG2E) - lse_s[u, 0:1, r]), 0.0)
            ps.append(p.astype(BF16))
            dss.append((p * (dpt[:, c] - del_s[u, 0:1, r])).astype(BF16))
    p = jnp.concatenate(ps, axis=1)
    ds = jnp.concatenate(dss, axis=1)
    dv = dot(p, g, 1, 0)
    dk = dot(ds, q, 1, 0)
    dq = dot(k, ds, 0, 0)
    for r in range(KB // T):
        piece = kb * (KB // T) + r
        rows = slice(r * T, (r + 1) * T)
        dkv_ref[piece, 0:T, :] += dk[rows]
        dkv_ref[piece, T : 2 * T, :] += dv[rows]
    for i, u in enumerate(us):
        dq_s[u] += dq[:, i * 2 * T : (i + 1) * 2 * T]


def turned(acc, u, h):
    return acc[u, :, h * T : (h + 1) * T].T * SCALE


def start_sums(dq_s, dkv_s):
    dq_s[...] = jnp.zeros_like(dq_s)
    dkv_s[...] = jnp.zeros_like(dkv_s)


def walk(q_ref, kv_ref, first, causal, dq_s, dkv_s, k_s, v_s, kid_s, lse_s, del_s, qid_s):
    fill_keys(kv_ref, first, k_s, v_s, kid_s)
    for qb in range(U // QP):
        head = qid_s[qb * QP, 0:1, 0:1]
        before = qb * QP if causal else U
        upto = (qb + 1) * QP if causal else U
        live = matching(kv_ref, first, head, before)

        @pl.loop((before * T - live) // KB, upto * T // KB)
        def _(kb, qb=qb):
            tile(q_ref, k_s, v_s, kid_s, lse_s, del_s, qid_s, dq_s, dkv_s, qb, kb, causal)


def near_kernel(q_ref, kv_ref, dq_ref, dprev_ref, down_ref, dq_s, *scratch):
    start_sums(dq_s, dprev_ref)
    down_ref[...] = jnp.zeros_like(down_ref)
    fill_rows(q_ref, *scratch[3:])
    walk(q_ref, kv_ref, KROWS, True, dq_s, down_ref, *scratch)
    walk(q_ref, kv_ref, 0, False, dq_s, dprev_ref, *scratch)
    for u in range(U):
        down_ref[u, 0:T, :] = down_ref[u, 0:T, :] * SCALE
        for h in range(2):
            dq_ref[u, h * T : (h + 1) * T, :] = turned(dq_s, u, h)


def far_kernel(q_ref, prev_ref, sum_ref, dq_ref, dkv_ref, dq_s, dkv_s, *scratch):
    dq_s[...] = jnp.zeros_like(dq_s)
    dkv_s[...] = sum_ref[...]
    fill_rows(q_ref, *scratch[3:])
    walk(q_ref, prev_ref, 0, False, dq_s, dkv_s, *scratch)
    for u in range(U):
        dkv_ref[u, 0:T, :] = (dkv_s[u, 0:T, :] * SCALE).astype(BF16)
        dkv_ref[u, T : 2 * T, :] = dkv_s[u, T : 2 * T, :].astype(BF16)
        for h in range(2):
            dq_ref[u, h * T : (h + 1) * T, :] = turned(dq_s, u, h).astype(BF16)


def total_kernel(dq_ref, more_q_ref, dkv_ref, more_kv_ref, out_ref):
    for u in range(U):
        out_ref[u, 0 : 2 * T, :] = (dq_ref[u] + more_q_ref[u].astype(F32)).astype(BF16)
        out_ref[u, 2 * T :, :] = (dkv_ref[u] + more_kv_ref[u].astype(F32)).astype(BF16)


def unpack_kernel(in_ref, q_ref, k_ref, v_ref):
    for j in range(U):
        for g in range(2):
            h = 2 * j + g
            q_ref[:, h * D : (h + 1) * D] = in_ref[j, g * T : (g + 1) * T, :]
        k_ref[:, j * D : (j + 1) * D] = in_ref[j, 2 * T : 3 * T, :]
        v_ref[:, j * D : (j + 1) * D] = in_ref[j, 3 * T : 4 * T, :]


def call(kernel, outs, scratch=(), flops=0, limit=16):
    many = isinstance(outs, tuple)
    return pl.pallas_call(
        kernel,
        out_shape=outs,
        out_specs=(VM,) * len(outs) if many else VM,
        scratch_shapes=scratch,
        cost_estimate=pl.CostEstimate(flops=flops, bytes_accessed=1 << 20, transcendentals=0),
        compiler_params=pltpu.CompilerParams(vmem_limit_bytes=limit << 20),
    )


KEYS = (
    pltpu.VMEM((U * T // KB, KB, D), BF16),
    pltpu.VMEM((U * T // KB, KB, D), BF16),
    pltpu.VMEM((U * T // KB, KB, D), F32),
    pltpu.VMEM((U, 8, 2 * T), F32),
    pltpu.VMEM((U, 8, 2 * T), F32),
    pltpu.VMEM((U, 8, T), F32),
)
SUM_Q = pltpu.VMEM((U, D, 2 * T), F32)
SUM_KV = pltpu.VMEM((U, 2 * T, D), F32)


def shape(*dims, dtype=BF16):
    return jax.ShapeDtypeStruct(dims, dtype)


def exchanged(message):
    return lax.all_to_all(message, ULY, 0, 0, tiled=True)


def moved(block, distance):
    count = lax.axis_size("blk")
    return lax.ppermute(block, "blk", [(i, (i + distance) % count) for i in range(count)])


def join_kernel(first_ref, second_ref, out_ref):
    out_ref[:, 0:KROWS, :] = first_ref[...]
    out_ref[:, KROWS:, :] = second_ref[...]


def stages(query, key, value, forward_out, out_grad, lse_parts, ids):
    ids = ids.reshape(1, T)
    kv_msg = call(pack_kv_kernel, shape(U, KROWS, D), flops=1 << 20, limit=56)(key, value, ids)
    prev_raw = moved(kv_msg, 1)
    message = call(pack_q_kernel, shape(U, QROWS, D), flops=1 << 20, limit=56)(
        query, out_grad, forward_out, lse_parts.transpose(1, 2, 0), ids
    )
    rows = exchanged(message)
    both = call(join_kernel, shape(U, 2 * KROWS, D), flops=1 << 20)(prev_raw, kv_msg)
    keys = exchanged(both)
    later_rows = moved(rows, -1)
    tall = shape(U, 2 * T, D, dtype=F32)
    dq, dprev, down = call(near_kernel, (tall, tall, tall), (SUM_Q,) + KEYS, flops=8 << 30)(rows, keys)
    half = shape(U, 2 * T, D)
    dq_msg, dkv_msg = call(far_kernel, (half, half), (SUM_Q, SUM_KV) + KEYS, flops=1 << 30)(
        later_rows, keys, dprev
    )
    total = call(total_kernel, shape(U, 4 * T, D), flops=1 << 20)(
        dq, moved(dq_msg, 1), down, moved(dkv_msg, -1)
    )
    return call(
        unpack_kernel, (shape(T, 2 * U * D), shape(T, U * D), shape(T, U * D)), flops=1 << 20
    )(exchanged(total))


def solution(mesh):
    torus = Mesh(mesh.devices.reshape(4, 2, mesh.shape["blk"]), ("uly_0", "uly_1", "blk"))
    flat, cube, line = P(BLK_ULY, None), P(BLK_ULY, None, None), P(BLK_ULY)
    return jax.shard_map(
        stages,
        mesh=torus,
        in_specs=(flat, flat, flat, flat, flat, cube, line),
        out_specs=(flat, flat, flat),
        check_vma=False,
    )
```

```python
import math

import jax
import jax.numpy as jnp
from jax import lax
from jax.experimental import pallas as pl
from jax.experimental.pallas import tpu as pltpu
from jax.sharding import Mesh
from jax.sharding import PartitionSpec as P


D = 128
T = 128
U = 8
KB = 256
QP = 2
STAT = 16
KROWS = 2 * T + STAT
QROWS = 4 * T + STAT
SCALE = 1.0 / math.sqrt(D)
LOG2E = 1.4426950408889634
ULY = ("uly_0", "uly_1")
BLK_ULY = ("blk", "uly_0", "uly_1")
F32 = jnp.float32
BF16 = jnp.bfloat16
VM = pl.BlockSpec(memory_space=pltpu.VMEM)


def dot(a, b, ca, cb):
    return lax.dot_general(a, b, (((ca,), (cb,)), ((), ())), preferred_element_type=F32)


def pack_kv_kernel(k_ref, v_ref, id_ref, out_ref):
    ids = jnp.broadcast_to(id_ref[...].astype(F32), (STAT, T)).astype(BF16)
    for j in range(U):
        out_ref[j, 0:T, :] = k_ref[:, j * D : (j + 1) * D]
        out_ref[j, T : 2 * T, :] = v_ref[:, j * D : (j + 1) * D]
        out_ref[j, 2 * T :, :] = ids


def three(x):
    hi = x.astype(BF16).astype(F32)
    rest = x - hi
    mid = rest.astype(BF16).astype(F32)
    return hi, mid, (rest - mid).astype(BF16).astype(F32)


def pack_q_kernel(q_ref, g_ref, o_ref, lse_ref, id_ref, out_ref):
    first, second = lse_ref[:, 0, :], lse_ref[:, 1, :]
    top = jnp.maximum(first, second)
    lse = top + jnp.log(jnp.exp(first - top) + jnp.exp(second - top))
    lane = lax.broadcasted_iota(jnp.int32, (T, D), 1)
    deltas = jnp.zeros((T, D), F32)
    for h in range(2 * U):
        cols = slice(h * D, (h + 1) * D)
        prod = g_ref[:, cols].astype(F32) * o_ref[:, cols].astype(F32)
        deltas = jnp.where(lane == h, jnp.sum(prod, axis=1, keepdims=True), deltas)
        j, g = divmod(h, 2)
        out_ref[j, g * T : (g + 1) * T, :] = q_ref[:, cols]
        out_ref[j, (2 + g) * T : (3 + g) * T, :] = g_ref[:, cols]
    parts = three(lse) + three(deltas.T)
    ids = jnp.broadcast_to(id_ref[...].astype(F32), (4, T))
    for j in range(U):
        rows = [p[2 * j : 2 * j + 2, :] for p in parts] + [ids]
        out_ref[j, 4 * T : QROWS, :] = jnp.concatenate(rows, axis=0).astype(BF16)


def fill_rows(q_ref, lse_s, del_s, qid_s):
    for u in range(U):
        st = q_ref[u, 4 * T : QROWS, :].astype(F32)
        two = st[0:2] + st[2:4] + st[4:6]
        dlt = st[6:8] + st[8:10] + st[10:12]
        for g in range(2):
            lse_s[u, 0:1, g * T : (g + 1) * T] = two[g : g + 1] * LOG2E
            del_s[u, 0:1, g * T : (g + 1) * T] = dlt[g : g + 1]
        qid_s[u, 0:1, :] = st[12:13]


def fill_keys(kv_ref, first, k_s, v_s, kid_s):
    pick = (lax.broadcasted_iota(jnp.int32, (STAT, D), 0) == 0).astype(F32).astype(BF16)
    for u in range(U):
        b, r = divmod(u, KB // T)
        rows = slice(r * T, (r + 1) * T)
        k_s[b, rows, :] = kv_ref[u, first : first + T, :]
        v_s[b, rows, :] = kv_ref[u, first + T : first + 2 * T, :]
        kid_s[b, rows, :] = dot(kv_ref[u, first + 2 * T : first + KROWS, :], pick, 0, 0)


def matching(kv_ref, first, qid, upto):
    total = jnp.zeros((1, T), F32)
    for u in range(upto):
        ids = kv_ref[u, first + 2 * T : first + 2 * T + 1, :].astype(F32)
        total = total + jnp.where(ids == qid, 1.0, 0.0)
    return jnp.sum(total).astype(jnp.int32)


def tile(q_ref, k_s, v_s, kid_s, lse_s, del_s, qid_s, dq_s, dkv_ref, qb, kb, causal):
    k, v = k_s[kb], v_s[kb]
    us = [qb * QP + i for i in range(QP)]
    q = jnp.concatenate([q_ref[u, 0 : 2 * T, :] for u in us], axis=0)
    g = jnp.concatenate([q_ref[u, 2 * T : 4 * T, :] for u in us], axis=0)
    st = dot(k, q, 1, 1)
    dpt = dot(v, g, 1, 1)
    kid = kid_s[kb]
    if causal:
        kpos = lax.broadcasted_iota(jnp.int32, (KB, T), 0) + kb * KB
        qpos = lax.broadcasted_iota(jnp.int32, (KB, T), 1)
    ps, dss = [], []
    for i, u in enumerate(us):
        okay = kid == qid_s[u, 0:1, :]
        if causal:
            okay = okay & (kpos <= qpos + u * T)
        for h in range(2):
            c = slice((2 * i + h) * T, (2 * i + h + 1) * T)
            r = slice(h * T, (h + 1) * T)
            p = jnp.where(okay, jnp.exp2(st[:, c] * (SCALE * LOG2E) - lse_s[u, 0:1, r]), 0.0)
            ps.append(p.astype(BF16))
            dss.append((p * (dpt[:, c] - del_s[u, 0:1, r])).astype(BF16))
    p = jnp.concatenate(ps, axis=1)
    ds = jnp.concatenate(dss, axis=1)
    dv = dot(p, g, 1, 0)
    dk = dot(ds, q, 1, 0)
    dq = dot(k, ds, 0, 0)
    for r in range(KB // T):
        piece = kb * (KB // T) + r
        rows = slice(r * T, (r + 1) * T)
        dkv_ref[piece, 0:T, :] += dk[rows]
        dkv_ref[piece, T : 2 * T, :] += dv[rows]
    for i, u in enumerate(us):
        dq_s[u] += dq[:, i * 2 * T : (i + 1) * 2 * T]


def turned(acc, u, h):
    return acc[u, :, h * T : (h + 1) * T].T * SCALE


def start_sums(dq_s, dkv_s):
    dq_s[...] = jnp.zeros_like(dq_s)
    dkv_s[...] = jnp.zeros_like(dkv_s)


def walk(q_ref, kv_ref, first, causal, dq_s, dkv_s, k_s, v_s, kid_s, lse_s, del_s, qid_s):
    fill_keys(kv_ref, first, k_s, v_s, kid_s)
    for qb in range(U // QP):
        head = qid_s[qb * QP, 0:1, 0:1]
        before = qb * QP if causal else U
        upto = (qb + 1) * QP if causal else U
        live = matching(kv_ref, first, head, before)

        @pl.loop((before * T - live) // KB, upto * T // KB)
        def _(kb, qb=qb):
            tile(q_ref, k_s, v_s, kid_s, lse_s, del_s, qid_s, dq_s, dkv_s, qb, kb, causal)


def prev_kernel(q_ref, kv_ref, dq_ref, dkv_ref, *scratch):
    start_sums(dq_ref, dkv_ref)
    fill_rows(q_ref, *scratch[3:])
    walk(q_ref, kv_ref, 0, False, dq_ref, dkv_ref, *scratch)


def own_kernel(q_ref, kv_ref, sum_ref, dq_ref, dkv_ref, dq_s, *scratch):
    dq_s[...] = sum_ref[...]
    dkv_ref[...] = jnp.zeros_like(dkv_ref)
    fill_rows(q_ref, *scratch[3:])
    walk(q_ref, kv_ref, KROWS, True, dq_s, dkv_ref, *scratch)
    for u in range(U):
        dkv_ref[u, 0:T, :] = dkv_ref[u, 0:T, :] * SCALE
        for h in range(2):
            dq_ref[u, h * T : (h + 1) * T, :] = turned(dq_s, u, h)


def far_kernel(q_ref, prev_ref, sum_ref, dq_ref, dkv_ref, dq_s, dkv_s, *scratch):
    dq_s[...] = jnp.zeros_like(dq_s)
    dkv_s[...] = sum_ref[...]
    fill_rows(q_ref, *scratch[3:])
    walk(q_ref, prev_ref, 0, False, dq_s, dkv_s, *scratch)
    for u in range(U):
        dkv_ref[u, 0:T, :] = (dkv_s[u, 0:T, :] * SCALE).astype(BF16)
        dkv_ref[u, T : 2 * T, :] = dkv_s[u, T : 2 * T, :].astype(BF16)
        for h in range(2):
            dq_ref[u, h * T : (h + 1) * T, :] = turned(dq_s, u, h).astype(BF16)


def total_kernel(dq_ref, more_q_ref, dkv_ref, more_kv_ref, out_ref):
    for u in range(U):
        out_ref[u, 0 : 2 * T, :] = (dq_ref[u] + more_q_ref[u].astype(F32)).astype(BF16)
        out_ref[u, 2 * T :, :] = (dkv_ref[u] + more_kv_ref[u].astype(F32)).astype(BF16)


def unpack_kernel(in_ref, q_ref, k_ref, v_ref):
    for j in range(U):
        for g in range(2):
            h = 2 * j + g
            q_ref[:, h * D : (h + 1) * D] = in_ref[j, g * T : (g + 1) * T, :]
        k_ref[:, j * D : (j + 1) * D] = in_ref[j, 2 * T : 3 * T, :]
        v_ref[:, j * D : (j + 1) * D] = in_ref[j, 3 * T : 4 * T, :]


def call(kernel, outs, scratch=(), flops=0, limit=16):
    many = isinstance(outs, tuple)
    return pl.pallas_call(
        kernel,
        out_shape=outs,
        out_specs=(VM,) * len(outs) if many else VM,
        scratch_shapes=scratch,
        cost_estimate=pl.CostEstimate(flops=flops, bytes_accessed=1 << 20, transcendentals=0),
        compiler_params=pltpu.CompilerParams(vmem_limit_bytes=limit << 20),
    )


KEYS = (
    pltpu.VMEM((U * T // KB, KB, D), BF16),
    pltpu.VMEM((U * T // KB, KB, D), BF16),
    pltpu.VMEM((U * T // KB, KB, D), F32),
    pltpu.VMEM((U, 8, 2 * T), F32),
    pltpu.VMEM((U, 8, 2 * T), F32),
    pltpu.VMEM((U, 8, T), F32),
)
SUM_Q = pltpu.VMEM((U, D, 2 * T), F32)
SUM_KV = pltpu.VMEM((U, 2 * T, D), F32)


def shape(*dims, dtype=BF16):
    return jax.ShapeDtypeStruct(dims, dtype)


def exchanged(message):
    return lax.all_to_all(message, ULY, 0, 0, tiled=True)


def moved(block, distance):
    count = lax.axis_size("blk")
    return lax.ppermute(block, "blk", [(i, (i + distance) % count) for i in range(count)])


def join_kernel(first_ref, second_ref, out_ref):
    out_ref[:, 0:KROWS, :] = first_ref[...]
    out_ref[:, KROWS:, :] = second_ref[...]


def stages(query, key, value, forward_out, out_grad, lse_parts, ids):
    ids = ids.reshape(1, T)
    message = call(pack_q_kernel, shape(U, QROWS, D), flops=1 << 20, limit=56)(
        query, out_grad, forward_out, lse_parts.transpose(1, 2, 0), ids
    )
    rows = exchanged(message)
    kv_msg = call(pack_kv_kernel, shape(U, KROWS, D), flops=1 << 20)(key, value, ids)
    prev_raw = moved(kv_msg, 1)
    later_rows = moved(rows, -1)
    both = call(join_kernel, shape(U, 2 * KROWS, D), flops=1 << 20)(prev_raw, kv_msg)
    keys = exchanged(both)
    tall, wide, half = shape(U, 2 * T, D, dtype=F32), shape(U, D, 2 * T, dtype=F32), shape(U, 2 * T, D)
    dq, dprev = call(prev_kernel, (wide, tall), KEYS, flops=4 << 30)(rows, keys)
    dq_msg, dkv_msg = call(far_kernel, (half, half), (SUM_Q, SUM_KV) + KEYS, flops=1 << 30)(later_rows, keys, dprev)
    dkv_back = moved(dkv_msg, -1)
    dq_back = moved(dq_msg, 1)
    dq, down = call(own_kernel, (tall, tall), (SUM_Q,) + KEYS, flops=4 << 30)(rows, keys, dq)
    total = call(total_kernel, shape(U, 4 * T, D), flops=1 << 20)(dq, dq_back, down, dkv_back)
    return call(unpack_kernel, (shape(T, 2 * U * D), shape(T, U * D), shape(T, U * D)), flops=1 << 20)(exchanged(total))


def solution(mesh):
    torus = Mesh(mesh.devices.reshape(4, 2, mesh.shape["blk"]), ("uly_0", "uly_1", "blk"))
    flat, cube, line = P(BLK_ULY, None), P(BLK_ULY, None, None), P(BLK_ULY)
    return jax.shard_map(
        stages,
        mesh=torus,
        in_specs=(flat, flat, flat, flat, flat, cube, line),
        out_specs=(flat, flat, flat),
        check_vma=False,
    )
```

```python
import math

import jax
import jax.numpy as jnp
from jax import lax
from jax.experimental import pallas as pl
from jax.experimental.pallas import tpu as pltpu
from jax.sharding import Mesh
from jax.sharding import PartitionSpec as P


D = 128
T = 128
U = 8
KB = 256
QP = 4
STAT = 16
KROWS = 2 * T + STAT
QROWS = 4 * T + STAT
SCALE = 1.0 / math.sqrt(D)
LOG2E = 1.4426950408889634
ULY = ("uly_0", "uly_1")
BLK_ULY = ("blk", "uly_0", "uly_1")
F32 = jnp.float32
BF16 = jnp.bfloat16
VM = pl.BlockSpec(memory_space=pltpu.VMEM)
FAR = pl.BlockSpec(memory_space=pl.ANY)


def dot(a, b, ca, cb):
    return lax.dot_general(a, b, (((ca,), (cb,)), ((), ())), preferred_element_type=F32)


def pack_kv_kernel(k_ref, v_ref, id_ref, out_ref):
    ids = jnp.broadcast_to(id_ref[...].astype(F32), (STAT, T)).astype(BF16)
    for j in range(U):
        out_ref[j, 0:T, :] = k_ref[:, j * D : (j + 1) * D]
        out_ref[j, T : 2 * T, :] = v_ref[:, j * D : (j + 1) * D]
        out_ref[j, 2 * T :, :] = ids


def three(x):
    hi = x.astype(BF16).astype(F32)
    rest = x - hi
    mid = rest.astype(BF16).astype(F32)
    return hi, mid, (rest - mid).astype(BF16).astype(F32)


def pack_q_kernel(q_ref, g_ref, o_ref, lse_ref, id_ref, out_ref, o_s, lse_s, id_s, sems, more_sems):
    def piece(ref, h, row, kind):
        j, g = divmod(h, 2)
        rows = pl.ds((row + g) * T, T)
        return pltpu.make_async_copy(ref.at[:, pl.ds(h * D, D)], out_ref.at[j, rows, :], sems.at[kind, h])

    grads = [piece(g_ref, h, 2, 0) for h in range(2 * U)]
    queries = [piece(q_ref, h, 0, 1) for h in range(2 * U)]
    outputs = [
        pltpu.make_async_copy(o_ref.at[:, pl.ds(h * D, D)], o_s.at[h], sems.at[2, h]) for h in range(2 * U)
    ]
    small = [
        pltpu.make_async_copy(lse_ref, lse_s, more_sems.at[0]),
        pltpu.make_async_copy(id_ref, id_s, more_sems.at[1]),
    ]
    for copy in small:
        copy.start()
    for h in range(2 * U):
        grads[h].start()
        outputs[h].start()
    for h in range(2 * U):
        queries[h].start()
    for copy in small:
        copy.wait()
    first, second = lse_s[:, 0, :], lse_s[:, 1, :]
    top = jnp.maximum(first, second)
    lse = top + jnp.log(jnp.exp(first - top) + jnp.exp(second - top))
    lane = lax.broadcasted_iota(jnp.int32, (T, D), 1)
    deltas = jnp.zeros((T, D), F32)
    for h in range(2 * U):
        j, g = divmod(h, 2)
        grads[h].wait()
        outputs[h].wait()
        prod = out_ref[j, (2 + g) * T : (3 + g) * T, :].astype(F32) * o_s[h].astype(F32)
        deltas = jnp.where(lane == h, jnp.sum(prod, axis=1, keepdims=True), deltas)
    parts = three(lse) + three(deltas.T)
    ids = jnp.broadcast_to(id_s[...].astype(F32), (4, T))
    for j in range(U):
        rows = [p[2 * j : 2 * j + 2, :] for p in parts] + [ids]
        out_ref[j, 4 * T : QROWS, :] = jnp.concatenate(rows, axis=0).astype(BF16)
    for copy in queries:
        copy.wait()


def fill_rows(q_ref, lse_s, del_s, qid_s):
    for u in range(U):
        st = q_ref[u, 4 * T : QROWS, :].astype(F32)
        two = st[0:2] + st[2:4] + st[4:6]
        dlt = st[6:8] + st[8:10] + st[10:12]
        for g in range(2):
            lse_s[u, 0:1, g * T : (g + 1) * T] = two[g : g + 1] * LOG2E
            del_s[u, 0:1, g * T : (g + 1) * T] = dlt[g : g + 1]
        qid_s[u, 0:1, :] = st[12:13]


def fill_keys(kv_ref, first, ids, k_s, v_s, kid_s):
    id_ref, start, row = ids
    pick = (lax.broadcasted_iota(jnp.int32, (STAT, D), 0) == row).astype(F32).astype(BF16)
    for u in range(U):
        b, r = divmod(u, KB // T)
        rows = slice(r * T, (r + 1) * T)
        k_s[b, rows, :] = kv_ref[u, first : first + T, :]
        v_s[b, rows, :] = kv_ref[u, first + T : first + 2 * T, :]
        kid_s[b, rows, :] = dot(id_ref[u, start : start + STAT, :], pick, 0, 0)


def matching(ids, qid, upto):
    id_ref, start, row = ids
    total = jnp.zeros((1, T), F32)
    for u in range(upto):
        here = id_ref[u, start : start + STAT, :].astype(F32)[row : row + 1]
        total = total + jnp.where(here == qid, 1.0, 0.0)
    return jnp.sum(total).astype(jnp.int32)


def tile(q_ref, k_s, v_s, kid_s, lse_s, del_s, qid_s, dq_s, dkv_ref, qb, kb, causal):
    k, v = k_s[kb], v_s[kb]
    us = [qb * QP + i for i in range(QP)]
    q = jnp.concatenate([q_ref[u, 0 : 2 * T, :] for u in us], axis=0)
    g = jnp.concatenate([q_ref[u, 2 * T : 4 * T, :] for u in us], axis=0)
    st = dot(k, q, 1, 1)
    dpt = dot(v, g, 1, 1)
    kid = kid_s[kb]
    if causal:
        kpos = lax.broadcasted_iota(jnp.int32, (KB, T), 0) + kb * KB
        qpos = lax.broadcasted_iota(jnp.int32, (KB, T), 1)
    ps, dss = [], []
    for i, u in enumerate(us):
        okay = kid == qid_s[u, 0:1, :]
        if causal:
            okay = okay & (kpos <= qpos + u * T)
        for h in range(2):
            c = slice((2 * i + h) * T, (2 * i + h + 1) * T)
            r = slice(h * T, (h + 1) * T)
            p = jnp.where(okay, jnp.exp2(st[:, c] * (SCALE * LOG2E) - lse_s[u, 0:1, r]), 0.0)
            ps.append(p.astype(BF16))
            dss.append((p * (dpt[:, c] - del_s[u, 0:1, r])).astype(BF16))
    p = jnp.concatenate(ps, axis=1)
    ds = jnp.concatenate(dss, axis=1)
    dv = dot(p, g, 1, 0)
    dk = dot(ds, q, 1, 0)
    dq = dot(k, ds, 0, 0)
    for r in range(KB // T):
        piece = kb * (KB // T) + r
        rows = slice(r * T, (r + 1) * T)
        dkv_ref[piece, 0:T, :] += dk[rows]
        dkv_ref[piece, T : 2 * T, :] += dv[rows]
    for i, u in enumerate(us):
        dq_s[u] += dq[:, i * 2 * T : (i + 1) * 2 * T]


def turned(acc, u, h):
    return acc[u, :, h * T : (h + 1) * T].T * SCALE


def start_sums(dq_s, dkv_s):
    dq_s[...] = jnp.zeros_like(dq_s)
    dkv_s[...] = jnp.zeros_like(dkv_s)


def walk(q_ref, kv_ref, first, ids, causal, dq_s, dkv_s, k_s, v_s, kid_s, lse_s, del_s, qid_s):
    fill_keys(kv_ref, first, ids, k_s, v_s, kid_s)
    for qb in range(U // QP):
        head = qid_s[qb * QP, 0:1, 0:1]
        before = qb * QP if causal else U
        upto = (qb + 1) * QP if causal else U
        live = matching(ids, head, before)

        @pl.loop((before * T - live) // KB, upto * T // KB)
        def _(kb, qb=qb):
            tile(q_ref, k_s, v_s, kid_s, lse_s, del_s, qid_s, dq_s, dkv_s, qb, kb, causal)


def prev_kernel(q_ref, kv_ref, dq_ref, dkv_ref, *scratch):
    start_sums(dq_ref, dkv_ref)
    fill_rows(q_ref, *scratch[3:])
    walk(q_ref, kv_ref, 0, (kv_ref, 2 * T, 0), False, dq_ref, dkv_ref, *scratch)


def own_kernel(q_ref, kv_ref, sum_ref, dq_ref, dkv_ref, dq_s, *scratch):
    dq_s[...] = sum_ref[...]
    dkv_ref[...] = jnp.zeros_like(dkv_ref)
    fill_rows(q_ref, *scratch[3:])
    walk(q_ref, kv_ref, KROWS, (q_ref, 4 * T, 12), True, dq_s, dkv_ref, *scratch)
    for u in range(U):
        dkv_ref[u, 0:T, :] = dkv_ref[u, 0:T, :] * SCALE
        for h in range(2):
            dq_ref[u, h * T : (h + 1) * T, :] = turned(dq_s, u, h)


def far_kernel(q_ref, prev_ref, sum_ref, dq_ref, dkv_ref, dq_s, dkv_s, *scratch):
    ids = (prev_ref, 2 * T, 0)
    head = q_ref[0, 4 * T : QROWS, :].astype(F32)[12:13, 0:1]
    some = matching(ids, head, U) > 0

    def leave(sums):
        for u in range(U):
            dkv_ref[u, 0:T, :] = (sums[u, 0:T, :] * SCALE).astype(BF16)
            dkv_ref[u, T : 2 * T, :] = sums[u, T : 2 * T, :].astype(BF16)

    @pl.when(some)
    def _():
        dq_s[...] = jnp.zeros_like(dq_s)
        dkv_s[...] = sum_ref[...]
        fill_rows(q_ref, *scratch[3:])
        walk(q_ref, prev_ref, 0, ids, False, dq_s, dkv_s, *scratch)
        leave(dkv_s)
        for u in range(U):
            for h in range(2):
                dq_ref[u, h * T : (h + 1) * T, :] = turned(dq_s, u, h).astype(BF16)

    @pl.when(jnp.logical_not(some))
    def _():
        leave(sum_ref)
        dq_ref[...] = jnp.zeros_like(dq_ref)


def total_kernel(dq_ref, more_q_ref, dkv_ref, more_kv_ref, out_ref):
    for u in range(U):
        out_ref[u, 0 : 2 * T, :] = (dq_ref[u] + more_q_ref[u].astype(F32)).astype(BF16)
        out_ref[u, 2 * T :, :] = (dkv_ref[u] + more_kv_ref[u].astype(F32)).astype(BF16)


def unpack_kernel(in_ref, q_ref, k_ref, v_ref, sems):
    copies = []
    for j in range(U):
        for part, (ref, block) in enumerate(((q_ref, 2 * j), (q_ref, 2 * j + 1), (k_ref, j), (v_ref, j))):
            source = in_ref.at[j, pl.ds(part * T, T), :]
            target = ref.at[:, pl.ds(block * D, D)]
            copies.append(pltpu.make_async_copy(source, target, sems.at[part, j]))
    for copy in copies:
        copy.start()
    for copy in copies:
        copy.wait()


def call(kernel, outs, scratch=(), flops=0, limit=16, far_in=(), far_out=False):
    many = isinstance(outs, tuple)
    spec = FAR if far_out else VM
    more = {"in_specs": [FAR if way else VM for way in far_in]} if far_in else {}
    return pl.pallas_call(
        kernel,
        out_shape=outs,
        out_specs=(spec,) * len(outs) if many else spec,
        **more,
        scratch_shapes=scratch,
        cost_estimate=pl.CostEstimate(flops=flops, bytes_accessed=1 << 20, transcendentals=0),
        compiler_params=pltpu.CompilerParams(vmem_limit_bytes=limit << 20),
    )


KEYS = (
    pltpu.VMEM((U * T // KB, KB, D), BF16),
    pltpu.VMEM((U * T // KB, KB, D), BF16),
    pltpu.VMEM((U * T // KB, KB, D), F32),
    pltpu.VMEM((U, 8, 2 * T), F32),
    pltpu.VMEM((U, 8, 2 * T), F32),
    pltpu.VMEM((U, 8, T), F32),
)
SUM_Q = pltpu.VMEM((U, D, 2 * T), F32)
SUM_KV = pltpu.VMEM((U, 2 * T, D), F32)


def shape(*dims, dtype=BF16):
    return jax.ShapeDtypeStruct(dims, dtype)


def exchanged(message):
    return lax.all_to_all(message, ULY, 0, 0, tiled=True)


def moved(block, distance):
    count = lax.axis_size("blk")
    return lax.ppermute(block, "blk", [(i, (i + distance) % count) for i in range(count)])


def join_kernel(first_ref, second_ref, out_ref):
    out_ref[:, 0:KROWS, :] = first_ref[...]
    out_ref[:, KROWS:, :] = second_ref[:, 0 : 2 * T, :]


def in_hbm(x):
    return pltpu.with_memory_space_constraint(x, pltpu.HBM)


def stages(query, key, value, forward_out, out_grad, lse_parts, ids):
    ids = ids.reshape(1, T)
    message = call(
        pack_q_kernel,
        shape(U, QROWS, D),
        [
            pltpu.VMEM((2 * U, T, D), BF16),
            pltpu.VMEM((2 * U, 2, T), F32),
            pltpu.VMEM((1, T), jnp.int32),
            pltpu.SemaphoreType.DMA((3, 2 * U)),
            pltpu.SemaphoreType.DMA((2,)),
        ],
        flops=1 << 20,
        far_in=(True,) * 5,
    )(*map(in_hbm, (query, out_grad, forward_out, lse_parts.transpose(1, 2, 0), ids)))
    rows = exchanged(message)
    kv_msg = call(pack_kv_kernel, shape(U, KROWS, D), flops=1 << 20)(key, value, ids)
    prev_raw = moved(kv_msg, 1)
    later_rows = moved(rows, -1)
    both = call(join_kernel, shape(U, KROWS + 2 * T, D), flops=1 << 20)(prev_raw, kv_msg)
    keys = exchanged(both)
    tall, wide, half = shape(U, 2 * T, D, dtype=F32), shape(U, D, 2 * T, dtype=F32), shape(U, 2 * T, D)
    dq, dprev = call(prev_kernel, (wide, tall), KEYS, flops=4 << 30)(rows, keys)
    dq_msg, dkv_msg = call(far_kernel, (half, half), (SUM_Q, SUM_KV) + KEYS, flops=1 << 30)(later_rows, keys, dprev)
    dkv_back = moved(dkv_msg, -1)
    dq_back = moved(dq_msg, 1)
    dq, down = call(own_kernel, (tall, tall), (SUM_Q,) + KEYS, flops=4 << 30)(rows, keys, dq)
    total = call(total_kernel, shape(U, 4 * T, D), flops=1 << 20)(dq, dq_back, down, dkv_back)
    return call(
        unpack_kernel,
        (shape(T, 2 * U * D), shape(T, U * D), shape(T, U * D)),
        [pltpu.SemaphoreType.DMA((4, U))],
        flops=1 << 20,
        far_in=(False,),
        far_out=True,
    )(exchanged(total))


def solution(mesh):
    torus = Mesh(mesh.devices.reshape(4, 2, mesh.shape["blk"]), ("uly_0", "uly_1", "blk"))
    flat, cube, line = P(BLK_ULY, None), P(BLK_ULY, None, None), P(BLK_ULY)
    return jax.shard_map(
        stages,
        mesh=torus,
        in_specs=(flat, flat, flat, flat, flat, cube, line),
        out_specs=(flat, flat, flat),
        check_vma=False,
    )
```

```python
import math

import jax
import jax.numpy as jnp
from jax import lax
from jax.experimental import pallas as pl
from jax.experimental.pallas import tpu as pltpu
from jax.sharding import Mesh
from jax.sharding import PartitionSpec as P


D = 128
T = 128
U = 8
KB = 256
QP = 4
FAR_QP = 2
STAT = 16
KROWS = 2 * T + STAT
QROWS = 4 * T + STAT
SCALE = 1.0 / math.sqrt(D)
LOG2E = 1.4426950408889634
ULY = ("uly_0", "uly_1")
BLK_ULY = ("blk", "uly_0", "uly_1")
F32 = jnp.float32
BF16 = jnp.bfloat16
VM = pl.BlockSpec(memory_space=pltpu.VMEM)


def dot(a, b, ca, cb):
    return lax.dot_general(a, b, (((ca,), (cb,)), ((), ())), preferred_element_type=F32)


def pack_kv_kernel(k_ref, v_ref, id_ref, out_ref):
    ids = jnp.broadcast_to(id_ref[...].astype(F32), (STAT, T)).astype(BF16)
    for j in range(U):
        out_ref[j, 0:T, :] = k_ref[:, j * D : (j + 1) * D]
        out_ref[j, T : 2 * T, :] = v_ref[:, j * D : (j + 1) * D]
        out_ref[j, 2 * T :, :] = ids


def three(x):
    hi = x.astype(BF16).astype(F32)
    rest = x - hi
    mid = rest.astype(BF16).astype(F32)
    return hi, mid, (rest - mid).astype(BF16).astype(F32)


def pack_q_kernel(q_ref, g_ref, o_ref, lse_ref, id_ref, out_ref):
    first, second = lse_ref[:, 0, :], lse_ref[:, 1, :]
    top = jnp.maximum(first, second)
    lse = top + jnp.log(jnp.exp(first - top) + jnp.exp(second - top))
    lane = lax.broadcasted_iota(jnp.int32, (T, D), 1)
    deltas = jnp.zeros((T, D), F32)
    for h in range(2 * U):
        cols = slice(h * D, (h + 1) * D)
        prod = g_ref[:, cols].astype(F32) * o_ref[:, cols].astype(F32)
        deltas = jnp.where(lane == h, jnp.sum(prod, axis=1, keepdims=True), deltas)
        j, g = divmod(h, 2)
        out_ref[j, g * T : (g + 1) * T, :] = q_ref[:, cols]
        out_ref[j, (2 + g) * T : (3 + g) * T, :] = g_ref[:, cols]
    parts = three(lse) + three(deltas.T)
    ids = jnp.broadcast_to(id_ref[...].astype(F32), (4, T))
    for j in range(U):
        rows = [p[2 * j : 2 * j + 2, :] for p in parts] + [ids]
        out_ref[j, 4 * T : QROWS, :] = jnp.concatenate(rows, axis=0).astype(BF16)


def fill_rows(q_ref, lse_s, del_s, qid_s):
    for u in range(U):
        st = q_ref[u, 4 * T : QROWS, :].astype(F32)
        two = st[0:2] + st[2:4] + st[4:6]
        dlt = st[6:8] + st[8:10] + st[10:12]
        for g in range(2):
            lse_s[u, 0:1, g * T : (g + 1) * T] = two[g : g + 1] * LOG2E
            del_s[u, 0:1, g * T : (g + 1) * T] = dlt[g : g + 1]
        qid_s[u, 0:1, :] = st[12:13]


def fill_keys(kv_ref, first, ids, k_s, v_s, kid_s):
    id_ref, start, row = ids
    pick = (lax.broadcasted_iota(jnp.int32, (STAT, D), 0) == row).astype(F32).astype(BF16)
    for u in range(U):
        b, r = divmod(u, KB // T)
        rows = slice(r * T, (r + 1) * T)
        k_s[b, rows, :] = kv_ref[u, first : first + T, :]
        v_s[b, rows, :] = kv_ref[u, first + T : first + 2 * T, :]
        kid_s[b, rows, :] = dot(id_ref[u, start : start + STAT, :], pick, 0, 0)


def matching(ids, qid, upto):
    id_ref, start, row = ids
    total = jnp.zeros((1, T), F32)
    for u in range(upto):
        here = id_ref[u, start : start + STAT, :].astype(F32)[row : row + 1]
        total = total + jnp.where(here == qid, 1.0, 0.0)
    return jnp.sum(total).astype(jnp.int32)


def tile(q_ref, k_s, v_s, kid_s, lse_s, del_s, qid_s, dq_s, dkv_ref, qb, kb, causal, qp):
    k, v = k_s[kb], v_s[kb]
    us = [qb * qp + i for i in range(qp)]
    q = jnp.concatenate([q_ref[u, 0 : 2 * T, :] for u in us], axis=0)
    g = jnp.concatenate([q_ref[u, 2 * T : 4 * T, :] for u in us], axis=0)
    st = dot(k, q, 1, 1)
    dpt = dot(v, g, 1, 1)
    kid = kid_s[kb]
    if causal:
        kpos = lax.broadcasted_iota(jnp.int32, (KB, T), 0) + kb * KB
        qpos = lax.broadcasted_iota(jnp.int32, (KB, T), 1)
    ps, dss = [], []
    for i, u in enumerate(us):
        okay = kid == qid_s[u, 0:1, :]
        if causal:
            okay = okay & (kpos <= qpos + u * T)
        for h in range(2):
            c = slice((2 * i + h) * T, (2 * i + h + 1) * T)
            r = slice(h * T, (h + 1) * T)
            p = jnp.where(okay, jnp.exp2(st[:, c] * (SCALE * LOG2E) - lse_s[u, 0:1, r]), 0.0)
            ps.append(p.astype(BF16))
            dss.append((p * (dpt[:, c] - del_s[u, 0:1, r])).astype(BF16))
    p = jnp.concatenate(ps, axis=1)
    ds = jnp.concatenate(dss, axis=1)
    dv = dot(p, g, 1, 0)
    dk = dot(ds, q, 1, 0)
    dq = dot(k, ds, 0, 0)
    for r in range(KB // T):
        piece = kb * (KB // T) + r
        rows = slice(r * T, (r + 1) * T)
        dkv_ref[piece, 0:T, :] += dk[rows]
        dkv_ref[piece, T : 2 * T, :] += dv[rows]
    for i, u in enumerate(us):
        dq_s[u] += dq[:, i * 2 * T : (i + 1) * 2 * T]


def turned(acc, u, h):
    return acc[u, :, h * T : (h + 1) * T].T * SCALE


def start_sums(dq_s, dkv_s):
    dq_s[...] = jnp.zeros_like(dq_s)
    dkv_s[...] = jnp.zeros_like(dkv_s)


def walk(qp, q_ref, kv_ref, first, ids, causal, dq_s, dkv_s, k_s, v_s, kid_s, lse_s, del_s, qid_s):
    fill_keys(kv_ref, first, ids, k_s, v_s, kid_s)
    for qb in range(U // qp):
        head = qid_s[qb * qp, 0:1, 0:1]
        before = qb * qp if causal else U
        upto = (qb + 1) * qp if causal else U
        live = matching(ids, head, before)

        @pl.loop((before * T - live) // KB, upto * T // KB)
        def _(kb, qb=qb):
            tile(q_ref, k_s, v_s, kid_s, lse_s, del_s, qid_s, dq_s, dkv_s, qb, kb, causal, qp)


def prev_kernel(q_ref, kv_ref, dq_ref, dkv_ref, *scratch):
    start_sums(dq_ref, dkv_ref)
    fill_rows(q_ref, *scratch[3:])
    walk(QP, q_ref, kv_ref, 0, (kv_ref, 2 * T, 0), False, dq_ref, dkv_ref, *scratch)


def own_kernel(q_ref, kv_ref, sum_ref, dq_ref, dkv_ref, dq_s, *scratch):
    dq_s[...] = sum_ref[...]
    dkv_ref[...] = jnp.zeros_like(dkv_ref)
    fill_rows(q_ref, *scratch[3:])
    walk(QP, q_ref, kv_ref, KROWS, (q_ref, 4 * T, 12), True, dq_s, dkv_ref, *scratch)
    for u in range(U):
        dkv_ref[u, 0:T, :] = dkv_ref[u, 0:T, :] * SCALE
        for h in range(2):
            dq_ref[u, h * T : (h + 1) * T, :] = turned(dq_s, u, h)


def far_kernel(q_ref, prev_ref, sum_ref, dq_ref, dkv_ref, dq_s, dkv_s, *scratch):
    ids = (prev_ref, 2 * T, 0)
    head = q_ref[0, 4 * T : QROWS, :].astype(F32)[12:13, 0:1]
    some = matching(ids, head, U) > 0

    def leave(sums):
        for u in range(U):
            dkv_ref[u, 0:T, :] = (sums[u, 0:T, :] * SCALE).astype(BF16)
            dkv_ref[u, T : 2 * T, :] = sums[u, T : 2 * T, :].astype(BF16)

    @pl.when(some)
    def _():
        dq_s[...] = jnp.zeros_like(dq_s)
        dkv_s[...] = sum_ref[...]
        fill_rows(q_ref, *scratch[3:])
        walk(FAR_QP, q_ref, prev_ref, 0, ids, False, dq_s, dkv_s, *scratch)
        leave(dkv_s)
        for u in range(U):
            for h in range(2):
                dq_ref[u, h * T : (h + 1) * T, :] = turned(dq_s, u, h).astype(BF16)

    @pl.when(jnp.logical_not(some))
    def _():
        leave(sum_ref)
        dq_ref[...] = jnp.zeros_like(dq_ref)


def total_kernel(dq_ref, more_q_ref, dkv_ref, more_kv_ref, out_ref):
    for u in range(U):
        out_ref[u, 0 : 2 * T, :] = (dq_ref[u] + more_q_ref[u].astype(F32)).astype(BF16)
        out_ref[u, 2 * T :, :] = (dkv_ref[u] + more_kv_ref[u].astype(F32)).astype(BF16)


def unpack_kernel(in_ref, q_ref, k_ref, v_ref):
    for j in range(U):
        for g in range(2):
            h = 2 * j + g
            q_ref[:, h * D : (h + 1) * D] = in_ref[j, g * T : (g + 1) * T, :]
        k_ref[:, j * D : (j + 1) * D] = in_ref[j, 2 * T : 3 * T, :]
        v_ref[:, j * D : (j + 1) * D] = in_ref[j, 3 * T : 4 * T, :]


def call(kernel, outs, scratch=(), flops=0, limit=16):
    many = isinstance(outs, tuple)
    return pl.pallas_call(
        kernel,
        out_shape=outs,
        out_specs=(VM,) * len(outs) if many else VM,
        scratch_shapes=scratch,
        cost_estimate=pl.CostEstimate(flops=flops, bytes_accessed=1 << 20, transcendentals=0),
        compiler_params=pltpu.CompilerParams(vmem_limit_bytes=limit << 20),
    )


KEYS = (
    pltpu.VMEM((U * T // KB, KB, D), BF16),
    pltpu.VMEM((U * T // KB, KB, D), BF16),
    pltpu.VMEM((U * T // KB, KB, D), F32),
    pltpu.VMEM((U, 8, 2 * T), F32),
    pltpu.VMEM((U, 8, 2 * T), F32),
    pltpu.VMEM((U, 8, T), F32),
)
SUM_Q = pltpu.VMEM((U, D, 2 * T), F32)
SUM_KV = pltpu.VMEM((U, 2 * T, D), F32)


def shape(*dims, dtype=BF16):
    return jax.ShapeDtypeStruct(dims, dtype)


def exchanged(message):
    return lax.all_to_all(message, ULY, 0, 0, tiled=True)


def moved(block, distance):
    count = lax.axis_size("blk")
    return lax.ppermute(block, "blk", [(i, (i + distance) % count) for i in range(count)])


def join_kernel(first_ref, second_ref, out_ref):
    out_ref[:, 0:KROWS, :] = first_ref[...]
    out_ref[:, KROWS:, :] = second_ref[:, 0 : 2 * T, :]


def in_hbm(x):
    return pltpu.with_memory_space_constraint(x, pltpu.HBM)


def stages(query, key, value, forward_out, out_grad, lse_parts, ids):
    ids = ids.reshape(1, T)
    message = call(pack_q_kernel, shape(U, QROWS, D), flops=1 << 20)(
        *map(in_hbm, (query, out_grad, forward_out, lse_parts.transpose(1, 2, 0), ids))
    )
    rows = exchanged(message)
    kv_msg = call(pack_kv_kernel, shape(U, KROWS, D), flops=1 << 20)(key, value, ids)
    prev_raw = moved(kv_msg, 1)
    later_rows = moved(rows, -1)
    both = call(join_kernel, shape(U, KROWS + 2 * T, D), flops=1 << 20)(prev_raw, kv_msg)
    keys = exchanged(both)
    tall, wide, half = shape(U, 2 * T, D, dtype=F32), shape(U, D, 2 * T, dtype=F32), shape(U, 2 * T, D)
    dq, dprev = call(prev_kernel, (wide, tall), KEYS, flops=4 << 30)(rows, keys)
    dq_msg, dkv_msg = call(far_kernel, (half, half), (SUM_Q, SUM_KV) + KEYS, flops=1 << 30)(later_rows, keys, dprev)
    dkv_back = moved(dkv_msg, -1)
    dq_back = moved(dq_msg, 1)
    dq, down = call(own_kernel, (tall, tall), (SUM_Q,) + KEYS, flops=4 << 30)(rows, keys, dq)
    total = call(total_kernel, shape(U, 4 * T, D), flops=1 << 20)(dq, dq_back, down, dkv_back)
    return call(unpack_kernel, (shape(T, 2 * U * D), shape(T, U * D), shape(T, U * D)), flops=1 << 20)(exchanged(total))


def solution(mesh):
    torus = Mesh(mesh.devices.reshape(4, 2, mesh.shape["blk"]), ("uly_0", "uly_1", "blk"))
    flat, cube, line = P(BLK_ULY, None), P(BLK_ULY, None, None), P(BLK_ULY)
    return jax.shard_map(
        stages,
        mesh=torus,
        in_specs=(flat, flat, flat, flat, flat, cube, line),
        out_specs=(flat, flat, flat),
        check_vma=False,
    )
```

```python
import functools
import math

import jax
import jax.numpy as jnp
from jax import lax
from jax.experimental import pallas as pl
from jax.experimental.pallas import tpu as pltpu
from jax.sharding import Mesh
from jax.sharding import PartitionSpec as P


D = 128
T = 128
U = 8
KB = 256
QP = 4
FAR_QP = 2
STAT = 16
KROWS = 2 * T + STAT
QROWS = 4 * T + STAT
SCALE = 1.0 / math.sqrt(D)
LOG2E = 1.4426950408889634
ULY = ("uly_0", "uly_1")
BLK_ULY = ("blk", "uly_0", "uly_1")
F32 = jnp.float32
BF16 = jnp.bfloat16
VM = pl.BlockSpec(memory_space=pltpu.VMEM)


def dot(a, b, ca, cb):
    return lax.dot_general(a, b, (((ca,), (cb,)), ((), ())), preferred_element_type=F32)


def pack_kv_kernel(k_ref, v_ref, id_ref, out_ref):
    ids = jnp.broadcast_to(id_ref[...].astype(F32), (STAT, T)).astype(BF16)
    for j in range(U):
        out_ref[j, 0:T, :] = k_ref[:, j * D : (j + 1) * D]
        out_ref[j, T : 2 * T, :] = v_ref[:, j * D : (j + 1) * D]
        out_ref[j, 2 * T :, :] = ids


def three(x):
    hi = x.astype(BF16).astype(F32)
    rest = x - hi
    mid = rest.astype(BF16).astype(F32)
    return hi, mid, (rest - mid).astype(BF16).astype(F32)


def pack_q_kernel(q_ref, g_ref, o_ref, lse_ref, id_ref, out_ref):
    first, second = lse_ref[:, 0, :], lse_ref[:, 1, :]
    top = jnp.maximum(first, second)
    lse = top + jnp.log(jnp.exp(first - top) + jnp.exp(second - top))
    lane = lax.broadcasted_iota(jnp.int32, (T, D), 1)
    deltas = jnp.zeros((T, D), F32)
    for h in range(2 * U):
        cols = slice(h * D, (h + 1) * D)
        prod = g_ref[:, cols].astype(F32) * o_ref[:, cols].astype(F32)
        deltas = jnp.where(lane == h, jnp.sum(prod, axis=1, keepdims=True), deltas)
        j, g = divmod(h, 2)
        out_ref[j, g * T : (g + 1) * T, :] = q_ref[:, cols]
        out_ref[j, (2 + g) * T : (3 + g) * T, :] = g_ref[:, cols]
    parts = three(lse) + three(deltas.T)
    ids = jnp.broadcast_to(id_ref[...].astype(F32), (4, T))
    for j in range(U):
        rows = [p[2 * j : 2 * j + 2, :] for p in parts] + [ids]
        out_ref[j, 4 * T : QROWS, :] = jnp.concatenate(rows, axis=0).astype(BF16)


def fill_rows(q_ref, lse_s, del_s, qid_s):
    for u in range(q_ref.shape[0]):
        st = q_ref[u, 4 * T : QROWS, :].astype(F32)
        two = st[0:2] + st[2:4] + st[4:6]
        dlt = st[6:8] + st[8:10] + st[10:12]
        for g in range(2):
            lse_s[u, 0:1, g * T : (g + 1) * T] = two[g : g + 1] * LOG2E
            del_s[u, 0:1, g * T : (g + 1) * T] = dlt[g : g + 1]
        qid_s[u, 0:1, :] = st[12:13]


def fill_keys(kv_ref, first, ids, k_s, v_s, kid_s):
    id_ref, start, row = ids
    pick = (lax.broadcasted_iota(jnp.int32, (STAT, D), 0) == row).astype(F32).astype(BF16)
    for u in range(U):
        b, r = divmod(u, KB // T)
        rows = slice(r * T, (r + 1) * T)
        k_s[b, rows, :] = kv_ref[u, first : first + T, :]
        v_s[b, rows, :] = kv_ref[u, first + T : first + 2 * T, :]
        kid_s[b, rows, :] = dot(id_ref[u, start : start + STAT, :], pick, 0, 0)


def matching(ids, qid, upto):
    id_ref, start, row = ids
    total = jnp.zeros((1, T), F32)
    for u in range(upto):
        here = id_ref[u, start : start + STAT, :].astype(F32)[row : row + 1]
        total = total + jnp.where(here == qid, 1.0, 0.0)
    return jnp.sum(total).astype(jnp.int32)


def tile(q_ref, k_s, v_s, kid_s, lse_s, del_s, qid_s, dq_s, dkv_ref, qb, kb, causal, qp):
    k, v = k_s[kb], v_s[kb]
    us = [qb * qp + i for i in range(qp)]
    q = jnp.concatenate([q_ref[u, 0 : 2 * T, :] for u in us], axis=0)
    g = jnp.concatenate([q_ref[u, 2 * T : 4 * T, :] for u in us], axis=0)
    st = dot(k, q, 1, 1)
    dpt = dot(v, g, 1, 1)
    kid = kid_s[kb]
    if causal:
        kpos = lax.broadcasted_iota(jnp.int32, (KB, T), 0) + kb * KB
        qpos = lax.broadcasted_iota(jnp.int32, (KB, T), 1)
    ps, dss = [], []
    for i, u in enumerate(us):
        okay = kid == qid_s[u, 0:1, :]
        if causal:
            okay = okay & (kpos <= qpos + u * T)
        for h in range(2):
            c = slice((2 * i + h) * T, (2 * i + h + 1) * T)
            r = slice(h * T, (h + 1) * T)
            p = jnp.where(okay, jnp.exp2(st[:, c] * (SCALE * LOG2E) - lse_s[u, 0:1, r]), 0.0)
            ps.append(p.astype(BF16))
            dss.append((p * (dpt[:, c] - del_s[u, 0:1, r])).astype(BF16))
    p = jnp.concatenate(ps, axis=1)
    ds = jnp.concatenate(dss, axis=1)
    dv = dot(p, g, 1, 0)
    dk = dot(ds, q, 1, 0)
    dq = dot(k, ds, 0, 0)
    for r in range(KB // T):
        piece = kb * (KB // T) + r
        rows = slice(r * T, (r + 1) * T)
        dkv_ref[piece, 0:T, :] += dk[rows]
        dkv_ref[piece, T : 2 * T, :] += dv[rows]
    for i, u in enumerate(us):
        dq_s[u] += dq[:, i * 2 * T : (i + 1) * 2 * T]


def turned(acc, u, h):
    return acc[u, :, h * T : (h + 1) * T].T * SCALE


def start_sums(dq_s, dkv_s):
    dq_s[...] = jnp.zeros_like(dq_s)
    dkv_s[...] = jnp.zeros_like(dkv_s)


def walk(qp, q_ref, kv_ref, first, ids, causal, dq_s, dkv_s, k_s, v_s, kid_s, lse_s, del_s, qid_s):
    fill_keys(kv_ref, first, ids, k_s, v_s, kid_s)
    for qb in range(q_ref.shape[0] // qp):
        head = qid_s[qb * qp, 0:1, 0:1]
        before = qb * qp if causal else U
        upto = (qb + 1) * qp if causal else U
        live = matching(ids, head, before)

        @pl.loop((before * T - live) // KB, upto * T // KB)
        def _(kb, qb=qb):
            tile(q_ref, k_s, v_s, kid_s, lse_s, del_s, qid_s, dq_s, dkv_s, qb, kb, causal, qp)


def prev_kernel(q_ref, kv_ref, dq_ref, dkv_ref, *scratch):
    start_sums(dq_ref, dkv_ref)
    fill_rows(q_ref, *scratch[3:])
    walk(QP, q_ref, kv_ref, 0, (kv_ref, 2 * T, 0), False, dq_ref, dkv_ref, *scratch)


def own_kernel(q_ref, kv_ref, sum_ref, dq_ref, dkv_ref, dq_s, *scratch):
    dq_s[...] = sum_ref[...]
    dkv_ref[...] = jnp.zeros_like(dkv_ref)
    fill_rows(q_ref, *scratch[3:])
    walk(QP, q_ref, kv_ref, KROWS, (q_ref, 4 * T, 12), True, dq_s, dkv_ref, *scratch)
    for u in range(U):
        dkv_ref[u, 0:T, :] = dkv_ref[u, 0:T, :] * SCALE
        for h in range(2):
            dq_ref[u, h * T : (h + 1) * T, :] = turned(dq_s, u, h)


def far_kernel(last, q_ref, prev_ref, sum_ref, dq_ref, dkv_ref, dq_s, dkv_s, *scratch):
    ids = (prev_ref, 2 * T, 0)
    head = q_ref[0, 4 * T : QROWS, :].astype(F32)[12:13, 0:1]
    some = matching(ids, head, U) > 0

    def leave(sums):
        for u in range(U):
            if last:
                dkv_ref[u, 0:T, :] = (sums[u, 0:T, :] * SCALE).astype(BF16)
                dkv_ref[u, T : 2 * T, :] = sums[u, T : 2 * T, :].astype(BF16)
            else:
                dkv_ref[u] = sums[u]

    @pl.when(some)
    def _():
        dq_s[...] = jnp.zeros_like(dq_s)
        dkv_s[...] = sum_ref[...]
        fill_rows(q_ref, *scratch[3:])
        walk(FAR_QP, q_ref, prev_ref, 0, ids, False, dq_s, dkv_s, *scratch)
        leave(dkv_s)
        for u in range(U // 2):
            for h in range(2):
                dq_ref[u, h * T : (h + 1) * T, :] = turned(dq_s, u, h).astype(BF16)

    @pl.when(jnp.logical_not(some))
    def _():
        leave(sum_ref)
        dq_ref[...] = jnp.zeros_like(dq_ref)


def total_kernel(dq_ref, front_ref, back_ref, dkv_ref, more_kv_ref, out_ref):
    for u in range(U):
        more_q = front_ref[u] if u < U // 2 else back_ref[u - U // 2]
        out_ref[u, 0 : 2 * T, :] = (dq_ref[u] + more_q.astype(F32)).astype(BF16)
        out_ref[u, 2 * T :, :] = (dkv_ref[u] + more_kv_ref[u].astype(F32)).astype(BF16)


def unpack_kernel(in_ref, q_ref, k_ref, v_ref):
    for j in range(U):
        for g in range(2):
            h = 2 * j + g
            q_ref[:, h * D : (h + 1) * D] = in_ref[j, g * T : (g + 1) * T, :]
        k_ref[:, j * D : (j + 1) * D] = in_ref[j, 2 * T : 3 * T, :]
        v_ref[:, j * D : (j + 1) * D] = in_ref[j, 3 * T : 4 * T, :]


def call(kernel, outs, scratch=(), flops=0, limit=16):
    many = isinstance(outs, tuple)
    return pl.pallas_call(
        kernel,
        out_shape=outs,
        out_specs=(VM,) * len(outs) if many else VM,
        scratch_shapes=scratch,
        cost_estimate=pl.CostEstimate(flops=flops, bytes_accessed=1 << 20, transcendentals=0),
        compiler_params=pltpu.CompilerParams(vmem_limit_bytes=limit << 20),
    )


KEYS = (
    pltpu.VMEM((U * T // KB, KB, D), BF16),
    pltpu.VMEM((U * T // KB, KB, D), BF16),
    pltpu.VMEM((U * T // KB, KB, D), F32),
    pltpu.VMEM((U, 8, 2 * T), F32),
    pltpu.VMEM((U, 8, 2 * T), F32),
    pltpu.VMEM((U, 8, T), F32),
)
SUM_Q = pltpu.VMEM((U, D, 2 * T), F32)
SUM_KV = pltpu.VMEM((U, 2 * T, D), F32)


def shape(*dims, dtype=BF16):
    return jax.ShapeDtypeStruct(dims, dtype)


def exchanged(message):
    return lax.all_to_all(message, ULY, 0, 0, tiled=True)


def moved(block, distance):
    count = lax.axis_size("blk")
    return lax.ppermute(block, "blk", [(i, (i + distance) % count) for i in range(count)])


def join_kernel(first_ref, second_ref, out_ref):
    out_ref[:, 0:KROWS, :] = first_ref[...]
    out_ref[:, KROWS:, :] = second_ref[:, 0 : 2 * T, :]


def in_hbm(x):
    return pltpu.with_memory_space_constraint(x, pltpu.HBM)


def stages(query, key, value, forward_out, out_grad, lse_parts, ids):
    ids = ids.reshape(1, T)
    message = call(pack_q_kernel, shape(U, QROWS, D), flops=1 << 20)(
        *map(in_hbm, (query, out_grad, forward_out, lse_parts.transpose(1, 2, 0), ids))
    )
    rows = exchanged(message)
    kv_msg = call(pack_kv_kernel, shape(U, KROWS, D), flops=1 << 20)(key, value, ids)
    prev_raw = moved(kv_msg, 1)
    front = moved(rows[: U // 2], -1)
    back = moved(rows[U // 2 :], -1)
    both = call(join_kernel, shape(U, KROWS + 2 * T, D), flops=1 << 20)(prev_raw, kv_msg)
    keys = exchanged(both)
    tall, wide, half = shape(U, 2 * T, D, dtype=F32), shape(U, D, 2 * T, dtype=F32), shape(U, 2 * T, D)
    dq, dprev = call(prev_kernel, (wide, tall), KEYS, flops=4 << 30)(rows, keys)
    part = shape(U // 2, 2 * T, D)
    sums = (pltpu.VMEM((U // 2, D, 2 * T), F32), SUM_KV) + KEYS
    dq_front, dprev = call(functools.partial(far_kernel, False), (part, tall), sums, flops=1 << 30)(front, keys, dprev)
    dq_front = moved(dq_front, 1)
    dq_tail, dkv_msg = call(functools.partial(far_kernel, True), (part, half), sums, flops=1 << 30)(back, keys, dprev)
    dkv_back = moved(dkv_msg, -1)
    dq_tail = moved(dq_tail, 1)
    dq, down = call(own_kernel, (tall, tall), (SUM_Q,) + KEYS, flops=4 << 30)(rows, keys, dq)
    total = call(total_kernel, shape(U, 4 * T, D), flops=1 << 20)(dq, dq_front, dq_tail, down, dkv_back)
    return call(unpack_kernel, (shape(T, 2 * U * D), shape(T, U * D), shape(T, U * D)), flops=1 << 20)(exchanged(total))


def solution(mesh):
    torus = Mesh(mesh.devices.reshape(4, 2, mesh.shape["blk"]), ("uly_0", "uly_1", "blk"))
    flat, cube, line = P(BLK_ULY, None), P(BLK_ULY, None, None), P(BLK_ULY)
    return jax.shard_map(
        stages,
        mesh=torus,
        in_specs=(flat, flat, flat, flat, flat, cube, line),
        out_specs=(flat, flat, flat),
        check_vma=False,
    )
```

```python
import math

import jax
import jax.numpy as jnp
from jax import lax
from jax.experimental import pallas as pl
from jax.experimental.pallas import tpu as pltpu
from jax.sharding import Mesh
from jax.sharding import PartitionSpec as P


D = 128
T = 128
U = 8
KB = 256
QP = 4
FAR_QP = 2
STAT = 16
KROWS = 2 * T + STAT
QROWS = 4 * T + STAT
SCALE = 1.0 / math.sqrt(D)
LOG2E = 1.4426950408889634
ULY = ("uly_0", "uly_1")
BLK_ULY = ("blk", "uly_0", "uly_1")
F32 = jnp.float32
BF16 = jnp.bfloat16
VM = pl.BlockSpec(memory_space=pltpu.VMEM)


def dot(a, b, ca, cb):
    return lax.dot_general(a, b, (((ca,), (cb,)), ((), ())), preferred_element_type=F32)


def pack_kv_kernel(k_ref, v_ref, id_ref, out_ref):
    ids = jnp.broadcast_to((id_ref[...] + 1).astype(F32), (STAT, T)).astype(BF16)
    for j in range(U):
        out_ref[j, 0:T, :] = k_ref[:, j * D : (j + 1) * D]
        out_ref[j, T : 2 * T, :] = v_ref[:, j * D : (j + 1) * D]
        out_ref[j, 2 * T :, :] = ids


def three(x):
    hi = x.astype(BF16).astype(F32)
    rest = x - hi
    mid = rest.astype(BF16).astype(F32)
    return hi, mid, (rest - mid).astype(BF16).astype(F32)


def pack_q_kernel(q_ref, g_ref, o_ref, lse_ref, id_ref, out_ref):
    first, second = lse_ref[:, 0, :], lse_ref[:, 1, :]
    top = jnp.maximum(first, second)
    lse = top + jnp.log(jnp.exp(first - top) + jnp.exp(second - top))
    lane = lax.broadcasted_iota(jnp.int32, (T, D), 1)
    deltas = jnp.zeros((T, D), F32)
    for h in range(2 * U):
        cols = slice(h * D, (h + 1) * D)
        prod = g_ref[:, cols].astype(F32) * o_ref[:, cols].astype(F32)
        deltas = jnp.where(lane == h, jnp.sum(prod, axis=1, keepdims=True), deltas)
        j, g = divmod(h, 2)
        out_ref[j, g * T : (g + 1) * T, :] = q_ref[:, cols]
        out_ref[j, (2 + g) * T : (3 + g) * T, :] = g_ref[:, cols]
    parts = three(lse) + three(deltas.T)
    ids = jnp.broadcast_to((id_ref[...] + 1).astype(F32), (4, T))
    for j in range(U):
        rows = [p[2 * j : 2 * j + 2, :] for p in parts] + [ids]
        out_ref[j, 4 * T : QROWS, :] = jnp.concatenate(rows, axis=0).astype(BF16)


def fill_rows(q_ref, lse_s, del_s, qid_s):
    for u in range(U):
        st = q_ref[u, 4 * T : QROWS, :].astype(F32)
        two = st[0:2] + st[2:4] + st[4:6]
        dlt = st[6:8] + st[8:10] + st[10:12]
        for g in range(2):
            lse_s[u, 0:1, g * T : (g + 1) * T] = two[g : g + 1] * LOG2E
            del_s[u, 0:1, g * T : (g + 1) * T] = dlt[g : g + 1]
        qid_s[u, 0:1, :] = st[12:13]


def fill_keys(kv_ref, first, ids, k_s, v_s, kid_s):
    id_ref, start, row = ids
    pick = (lax.broadcasted_iota(jnp.int32, (STAT, D), 0) == row).astype(F32).astype(BF16)
    for u in range(U):
        b, r = divmod(u, KB // T)
        rows = slice(r * T, (r + 1) * T)
        k_s[b, rows, :] = kv_ref[u, first : first + T, :]
        v_s[b, rows, :] = kv_ref[u, first + T : first + 2 * T, :]
        kid_s[b, rows, :] = dot(id_ref[u, start : start + STAT, :], pick, 0, 0)


def matching(ids, qid, upto):
    id_ref, start, row = ids
    total = jnp.zeros((1, T), F32)
    for u in range(upto):
        here = id_ref[u, start : start + STAT, :].astype(F32)[row : row + 1]
        total = total + jnp.where(here == qid, 1.0, 0.0)
    return jnp.sum(total).astype(jnp.int32)


def tile(q_ref, k_s, v_s, kid_s, lse_s, del_s, qid_s, dq_s, dkv_ref, qb, kb, causal, qp):
    k, v = k_s[kb], v_s[kb]
    us = [qb * qp + i for i in range(qp)]
    q = jnp.concatenate([q_ref[u, 0 : 2 * T, :] for u in us], axis=0)
    g = jnp.concatenate([q_ref[u, 2 * T : 4 * T, :] for u in us], axis=0)
    st = dot(k, q, 1, 1)
    dpt = dot(v, g, 1, 1)
    kid = kid_s[kb]
    if causal:
        kpos = lax.broadcasted_iota(jnp.int32, (KB, T), 0) + kb * KB
        qpos = lax.broadcasted_iota(jnp.int32, (KB, T), 1)
    ps, dss = [], []
    for i, u in enumerate(us):
        okay = kid == qid_s[u, 0:1, :]
        if causal:
            okay = okay & (kpos <= qpos + u * T)
        for h in range(2):
            c = slice((2 * i + h) * T, (2 * i + h + 1) * T)
            r = slice(h * T, (h + 1) * T)
            p = jnp.where(okay, jnp.exp2(st[:, c] * (SCALE * LOG2E) - lse_s[u, 0:1, r]), 0.0)
            ps.append(p.astype(BF16))
            dss.append((p * (dpt[:, c] - del_s[u, 0:1, r])).astype(BF16))
    p = jnp.concatenate(ps, axis=1)
    ds = jnp.concatenate(dss, axis=1)
    dv = dot(p, g, 1, 0)
    dk = dot(ds, q, 1, 0)
    dq = dot(k, ds, 0, 0)
    for r in range(KB // T):
        piece = kb * (KB // T) + r
        rows = slice(r * T, (r + 1) * T)
        dkv_ref[piece, 0:T, :] += dk[rows]
        dkv_ref[piece, T : 2 * T, :] += dv[rows]
    for i, u in enumerate(us):
        dq_s[u] += dq[:, i * 2 * T : (i + 1) * 2 * T]


def turned(acc, u, h):
    return acc[u, :, h * T : (h + 1) * T].T * SCALE


def start_sums(dq_s, dkv_s):
    dq_s[...] = jnp.zeros_like(dq_s)
    dkv_s[...] = jnp.zeros_like(dkv_s)


def walk(qp, q_ref, kv_ref, first, ids, causal, dq_s, dkv_s, k_s, v_s, kid_s, lse_s, del_s, qid_s):
    fill_keys(kv_ref, first, ids, k_s, v_s, kid_s)
    for qb in range(U // qp):
        head = qid_s[qb * qp, 0:1, 0:1]
        before = qb * qp if causal else U
        upto = (qb + 1) * qp if causal else U
        live = matching(ids, head, before)

        @pl.loop((before * T - live) // KB, upto * T // KB)
        def _(kb, qb=qb):
            tile(q_ref, k_s, v_s, kid_s, lse_s, del_s, qid_s, dq_s, dkv_s, qb, kb, causal, qp)


def prev_kernel(q_ref, kv_ref, dq_ref, dkv_ref, *scratch):
    start_sums(dq_ref, dkv_ref)
    fill_rows(q_ref, *scratch[3:])
    walk(QP, q_ref, kv_ref, 0, (kv_ref, 2 * T, 0), False, dq_ref, dkv_ref, *scratch)


def own_kernel(q_ref, kv_ref, sum_ref, dq_ref, dkv_ref, dq_s, *scratch):
    dq_s[...] = sum_ref[...]
    dkv_ref[...] = jnp.zeros_like(dkv_ref)
    fill_rows(q_ref, *scratch[3:])
    walk(QP, q_ref, kv_ref, KROWS, (q_ref, 4 * T, 12), True, dq_s, dkv_ref, *scratch)
    for u in range(U):
        dkv_ref[u, 0:T, :] = dkv_ref[u, 0:T, :] * SCALE
        for h in range(2):
            dq_ref[u, h * T : (h + 1) * T, :] = turned(dq_s, u, h)


def far_kernel(q_ref, prev_ref, sum_ref, dq_ref, dkv_ref, dq_s, dkv_s, *scratch):
    ids = (prev_ref, 2 * T, 0)
    head = q_ref[0, 4 * T : QROWS, :].astype(F32)[12:13, 0:1]
    some = matching(ids, head, U) > 0

    def leave(sums):
        for u in range(U):
            dkv_ref[u, 0:T, :] = (sums[u, 0:T, :] * SCALE).astype(BF16)
            dkv_ref[u, T : 2 * T, :] = sums[u, T : 2 * T, :].astype(BF16)

    @pl.when(some)
    def _():
        dq_s[...] = jnp.zeros_like(dq_s)
        dkv_s[...] = sum_ref[...]
        fill_rows(q_ref, *scratch[3:])
        walk(FAR_QP, q_ref, prev_ref, 0, ids, False, dq_s, dkv_s, *scratch)
        leave(dkv_s)
        for u in range(U):
            for h in range(2):
                dq_ref[u, h * T : (h + 1) * T, :] = turned(dq_s, u, h).astype(BF16)

    @pl.when(jnp.logical_not(some))
    def _():
        leave(sum_ref)
        dq_ref[...] = jnp.zeros_like(dq_ref)


def total_kernel(dq_ref, more_q_ref, dkv_ref, more_kv_ref, out_ref):
    for u in range(U):
        out_ref[u, 0 : 2 * T, :] = (dq_ref[u] + more_q_ref[u].astype(F32)).astype(BF16)
        out_ref[u, 2 * T :, :] = (dkv_ref[u] + more_kv_ref[u].astype(F32)).astype(BF16)


def unpack_kernel(in_ref, q_ref, k_ref, v_ref):
    for j in range(U):
        for g in range(2):
            h = 2 * j + g
            q_ref[:, h * D : (h + 1) * D] = in_ref[j, g * T : (g + 1) * T, :]
        k_ref[:, j * D : (j + 1) * D] = in_ref[j, 2 * T : 3 * T, :]
        v_ref[:, j * D : (j + 1) * D] = in_ref[j, 3 * T : 4 * T, :]


def call(kernel, outs, scratch=(), flops=0, limit=16):
    many = isinstance(outs, tuple)
    return pl.pallas_call(
        kernel,
        out_shape=outs,
        out_specs=(VM,) * len(outs) if many else VM,
        scratch_shapes=scratch,
        cost_estimate=pl.CostEstimate(flops=flops, bytes_accessed=1 << 20, transcendentals=0),
        compiler_params=pltpu.CompilerParams(vmem_limit_bytes=limit << 20),
    )


KEYS = (
    pltpu.VMEM((U * T // KB, KB, D), BF16),
    pltpu.VMEM((U * T // KB, KB, D), BF16),
    pltpu.VMEM((U * T // KB, KB, D), F32),
    pltpu.VMEM((U, 8, 2 * T), F32),
    pltpu.VMEM((U, 8, 2 * T), F32),
    pltpu.VMEM((U, 8, T), F32),
)
SUM_Q = pltpu.VMEM((U, D, 2 * T), F32)
SUM_KV = pltpu.VMEM((U, 2 * T, D), F32)


def shape(*dims, dtype=BF16):
    return jax.ShapeDtypeStruct(dims, dtype)


def exchanged(message):
    return lax.all_to_all(message, ULY, 0, 0, tiled=True)


def moved(block, distance):
    count = lax.axis_size("blk")
    route = [(i, i + distance) for i in range(count) if 0 <= i + distance < count]
    return lax.ppermute(block, "blk", route)


def join_kernel(first_ref, second_ref, out_ref):
    out_ref[:, 0:KROWS, :] = first_ref[...]
    out_ref[:, KROWS:, :] = second_ref[:, 0 : 2 * T, :]


def in_hbm(x):
    return pltpu.with_memory_space_constraint(x, pltpu.HBM)


def stages(query, key, value, forward_out, out_grad, lse_parts, ids):
    ids = ids.reshape(1, T)
    message = call(pack_q_kernel, shape(U, QROWS, D), flops=1 << 20)(
        *map(in_hbm, (query, out_grad, forward_out, lse_parts.transpose(1, 2, 0), ids))
    )
    rows = exchanged(message)
    kv_msg = call(pack_kv_kernel, shape(U, KROWS, D), flops=1 << 20)(key, value, ids)
    prev_raw = moved(kv_msg, 1)
    later_rows = moved(rows, -1)
    both = call(join_kernel, shape(U, KROWS + 2 * T, D), flops=1 << 20)(prev_raw, kv_msg)
    keys = exchanged(both)
    tall, wide, half = shape(U, 2 * T, D, dtype=F32), shape(U, D, 2 * T, dtype=F32), shape(U, 2 * T, D)
    dq, dprev = call(prev_kernel, (wide, tall), KEYS, flops=4 << 30)(rows, keys)
    dq_msg, dkv_msg = call(far_kernel, (half, half), (SUM_Q, SUM_KV) + KEYS, flops=1 << 30)(later_rows, keys, dprev)
    dkv_back = moved(dkv_msg, -1)
    dq_back = moved(dq_msg, 1)
    dq, down = call(own_kernel, (tall, tall), (SUM_Q,) + KEYS, flops=4 << 30)(rows, keys, dq)
    total = call(total_kernel, shape(U, 4 * T, D), flops=1 << 20)(dq, dq_back, down, dkv_back)
    return call(unpack_kernel, (shape(T, 2 * U * D), shape(T, U * D), shape(T, U * D)), flops=1 << 20)(exchanged(total))


def solution(mesh):
    torus = Mesh(mesh.devices.reshape(4, 2, mesh.shape["blk"]), ("uly_0", "uly_1", "blk"))
    flat, cube, line = P(BLK_ULY, None), P(BLK_ULY, None, None), P(BLK_ULY)
    return jax.shard_map(
        stages,
        mesh=torus,
        in_specs=(flat, flat, flat, flat, flat, cube, line),
        out_specs=(flat, flat, flat),
        check_vma=False,
    )
```

```python
import math

import jax
import jax.numpy as jnp
from jax import lax
from jax.experimental import pallas as pl
from jax.experimental.pallas import tpu as pltpu
from jax.sharding import Mesh
from jax.sharding import PartitionSpec as P


D = 128
T = 128
U = 8
KB = 256
QP = 4
FAR_QP = 2
STAT = 16
KROWS = 2 * T + STAT
QROWS = 4 * T + STAT
SCALE = 1.0 / math.sqrt(D)
LOG2E = 1.4426950408889634
ULY = ("uly_0", "uly_1")
BLK_ULY = ("blk", "uly_0", "uly_1")
F32 = jnp.float32
BF16 = jnp.bfloat16
VM = pl.BlockSpec(memory_space=pltpu.VMEM)


def dot(a, b, ca, cb):
    return lax.dot_general(a, b, (((ca,), (cb,)), ((), ())), preferred_element_type=F32)


def pack_kv_kernel(k_ref, v_ref, id_ref, out_ref):
    ids = jnp.broadcast_to((id_ref[...] + 1).astype(F32), (STAT, T)).astype(BF16)
    for j in range(U):
        out_ref[j, 0:T, :] = k_ref[:, j * D : (j + 1) * D]
        out_ref[j, T : 2 * T, :] = v_ref[:, j * D : (j + 1) * D]
        out_ref[j, 2 * T :, :] = ids


def three(x):
    hi = x.astype(BF16).astype(F32)
    rest = x - hi
    mid = rest.astype(BF16).astype(F32)
    return hi, mid, (rest - mid).astype(BF16).astype(F32)


def pack_q_kernel(q_ref, g_ref, o_ref, lse_ref, id_ref, out_ref):
    first, second = lse_ref[:, 0, :], lse_ref[:, 1, :]
    top = jnp.maximum(first, second)
    lse = top + jnp.log(jnp.exp(first - top) + jnp.exp(second - top))
    lane = lax.broadcasted_iota(jnp.int32, (T, D), 1)
    deltas = jnp.zeros((T, D), F32)
    for h in range(2 * U):
        cols = slice(h * D, (h + 1) * D)
        prod = g_ref[:, cols].astype(F32) * o_ref[:, cols].astype(F32)
        deltas = jnp.where(lane == h, jnp.sum(prod, axis=1, keepdims=True), deltas)
        j, g = divmod(h, 2)
        out_ref[j, g * T : (g + 1) * T, :] = q_ref[:, cols]
        out_ref[j, (2 + g) * T : (3 + g) * T, :] = g_ref[:, cols]
    parts = three(lse) + three(deltas.T)
    ids = jnp.broadcast_to((id_ref[...] + 1).astype(F32), (4, T))
    for j in range(U):
        rows = [p[2 * j : 2 * j + 2, :] for p in parts] + [ids]
        out_ref[j, 4 * T : QROWS, :] = jnp.concatenate(rows, axis=0).astype(BF16)


def fill_rows(q_ref, lse_s, del_s, qid_s):
    for u in range(U):
        st = q_ref[u, 4 * T : QROWS, :].astype(F32)
        two = st[0:2] + st[2:4] + st[4:6]
        dlt = st[6:8] + st[8:10] + st[10:12]
        for g in range(2):
            lse_s[u, 0:1, g * T : (g + 1) * T] = two[g : g + 1] * LOG2E
            del_s[u, 0:1, g * T : (g + 1) * T] = dlt[g : g + 1]
        qid_s[u, 0:1, :] = st[12:13]


def fill_keys(kv_ref, first, ids, k_s, v_s, kid_s):
    id_ref, start, row = ids
    pick = (lax.broadcasted_iota(jnp.int32, (STAT, D), 0) == row).astype(F32).astype(BF16)
    for u in range(U):
        b, r = divmod(u, KB // T)
        rows = slice(r * T, (r + 1) * T)
        k_s[b, rows, :] = kv_ref[u, first : first + T, :]
        v_s[b, rows, :] = kv_ref[u, first + T : first + 2 * T, :]
        kid_s[b, rows, :] = dot(id_ref[u, start : start + STAT, :], pick, 0, 0)


def matching(ids, qid, upto):
    id_ref, start, row = ids
    total = jnp.zeros((1, T), F32)
    for u in range(upto):
        here = id_ref[u, start : start + STAT, :].astype(F32)[row : row + 1]
        total = total + jnp.where(here == qid, 1.0, 0.0)
    return jnp.sum(total).astype(jnp.int32)


def tile(q_ref, k_s, v_s, kid_s, lse_s, del_s, qid_s, dq_s, dkv_ref, qb, kb, causal, qp):
    k, v = k_s[kb], v_s[kb]
    us = [qb * qp + i for i in range(qp)]
    q = jnp.concatenate([q_ref[u, 0 : 2 * T, :] for u in us], axis=0)
    g = jnp.concatenate([q_ref[u, 2 * T : 4 * T, :] for u in us], axis=0)
    st = dot(k, q, 1, 1)
    dpt = dot(v, g, 1, 1)
    kid = kid_s[kb]
    if causal:
        kpos = lax.broadcasted_iota(jnp.int32, (KB, T), 0) + kb * KB
        qpos = lax.broadcasted_iota(jnp.int32, (KB, T), 1)
    ps, dss = [], []
    for i, u in enumerate(us):
        okay = kid == qid_s[u, 0:1, :]
        if causal:
            okay = okay & (kpos <= qpos + u * T)
        for h in range(2):
            c = slice((2 * i + h) * T, (2 * i + h + 1) * T)
            r = slice(h * T, (h + 1) * T)
            p = jnp.where(okay, jnp.exp2(st[:, c] * (SCALE * LOG2E) - lse_s[u, 0:1, r]), 0.0)
            ps.append(p.astype(BF16))
            dss.append((p * (dpt[:, c] - del_s[u, 0:1, r])).astype(BF16))
    p = jnp.concatenate(ps, axis=1)
    ds = jnp.concatenate(dss, axis=1)
    dv = dot(p, g, 1, 0)
    dk = dot(ds, q, 1, 0)
    dq = dot(k, ds, 0, 0)
    for r in range(KB // T):
        piece = kb * (KB // T) + r
        rows = slice(r * T, (r + 1) * T)
        dkv_ref[piece, 0:T, :] += dk[rows]
        dkv_ref[piece, T : 2 * T, :] += dv[rows]
    for i, u in enumerate(us):
        dq_s[u] += dq[:, i * 2 * T : (i + 1) * 2 * T]


def turned(acc, u, h):
    return acc[u, :, h * T : (h + 1) * T].T * SCALE


def start_sums(dq_s, dkv_s):
    dq_s[...] = jnp.zeros_like(dq_s)
    dkv_s[...] = jnp.zeros_like(dkv_s)


def walk(qp, q_ref, kv_ref, first, ids, causal, dq_s, dkv_s, k_s, v_s, kid_s, lse_s, del_s, qid_s):
    fill_keys(kv_ref, first, ids, k_s, v_s, kid_s)
    for qb in range(U // qp):
        head = qid_s[qb * qp, 0:1, 0:1]
        before = qb * qp if causal else U
        upto = (qb + 1) * qp if causal else U
        live = matching(ids, head, before)

        @pl.loop((before * T - live) // KB, upto * T // KB)
        def _(kb, qb=qb):
            tile(q_ref, k_s, v_s, kid_s, lse_s, del_s, qid_s, dq_s, dkv_s, qb, kb, causal, qp)


def walk_back(q_ref, kv_ref, first, ids, dq_s, dkv_s, k_s, v_s, kid_s, lse_s, del_s, qid_s):
    fill_keys(kv_ref, first, ids, k_s, v_s, kid_s)
    end = U * T // KB
    for qb in range(U // QP):
        front = matching(ids, qid_s[qb * QP, 0:1, 0:1], U)
        back = matching(ids, qid_s[qb * QP + FAR_QP, 0:1, 0:1], U)
        start = (U * T - front) // KB

        @pl.loop(jnp.where(back > 0, start, end), end)
        def _(kb, qb=qb):
            tile(q_ref, k_s, v_s, kid_s, lse_s, del_s, qid_s, dq_s, dkv_s, qb, kb, False, QP)

        @pl.loop(jnp.where(back > 0, end, start), end)
        def _(kb, qb=qb):
            tile(q_ref, k_s, v_s, kid_s, lse_s, del_s, qid_s, dq_s, dkv_s, 2 * qb, kb, False, FAR_QP)


def prev_kernel(q_ref, kv_ref, dq_ref, dkv_ref, *scratch):
    start_sums(dq_ref, dkv_ref)
    fill_rows(q_ref, *scratch[3:])
    walk_back(q_ref, kv_ref, 0, (kv_ref, 2 * T, 0), dq_ref, dkv_ref, *scratch)


def own_kernel(q_ref, kv_ref, sum_ref, dq_ref, dkv_ref, dq_s, *scratch):
    dq_s[...] = sum_ref[...]
    dkv_ref[...] = jnp.zeros_like(dkv_ref)
    fill_rows(q_ref, *scratch[3:])
    walk(QP, q_ref, kv_ref, KROWS, (q_ref, 4 * T, 12), True, dq_s, dkv_ref, *scratch)
    for u in range(U):
        dkv_ref[u, 0:T, :] = dkv_ref[u, 0:T, :] * SCALE
        for h in range(2):
            dq_ref[u, h * T : (h + 1) * T, :] = turned(dq_s, u, h)


def far_kernel(q_ref, prev_ref, sum_ref, dq_ref, dkv_ref, dq_s, dkv_s, *scratch):
    ids = (prev_ref, 2 * T, 0)
    head = q_ref[0, 4 * T : QROWS, :].astype(F32)[12:13, 0:1]
    some = matching(ids, head, U) > 0

    def leave(sums):
        for u in range(U):
            dkv_ref[u, 0:T, :] = (sums[u, 0:T, :] * SCALE).astype(BF16)
            dkv_ref[u, T : 2 * T, :] = sums[u, T : 2 * T, :].astype(BF16)

    @pl.when(some)
    def _():
        dq_s[...] = jnp.zeros_like(dq_s)
        dkv_s[...] = sum_ref[...]
        fill_rows(q_ref, *scratch[3:])
        walk_back(q_ref, prev_ref, 0, ids, dq_s, dkv_s, *scratch)
        leave(dkv_s)
        for u in range(U):
            for h in range(2):
                dq_ref[u, h * T : (h + 1) * T, :] = turned(dq_s, u, h).astype(BF16)

    @pl.when(jnp.logical_not(some))
    def _():
        leave(sum_ref)
        dq_ref[...] = jnp.zeros_like(dq_ref)


def total_kernel(dq_ref, more_q_ref, dkv_ref, more_kv_ref, out_ref):
    for u in range(U):
        out_ref[u, 0 : 2 * T, :] = (dq_ref[u] + more_q_ref[u].astype(F32)).astype(BF16)
        out_ref[u, 2 * T :, :] = (dkv_ref[u] + more_kv_ref[u].astype(F32)).astype(BF16)


def unpack_kernel(in_ref, q_ref, k_ref, v_ref):
    for j in range(U):
        for g in range(2):
            h = 2 * j + g
            q_ref[:, h * D : (h + 1) * D] = in_ref[j, g * T : (g + 1) * T, :]
        k_ref[:, j * D : (j + 1) * D] = in_ref[j, 2 * T : 3 * T, :]
        v_ref[:, j * D : (j + 1) * D] = in_ref[j, 3 * T : 4 * T, :]


def call(kernel, outs, scratch=(), flops=0, limit=16):
    many = isinstance(outs, tuple)
    return pl.pallas_call(
        kernel,
        out_shape=outs,
        out_specs=(VM,) * len(outs) if many else VM,
        scratch_shapes=scratch,
        cost_estimate=pl.CostEstimate(flops=flops, bytes_accessed=1 << 20, transcendentals=0),
        compiler_params=pltpu.CompilerParams(vmem_limit_bytes=limit << 20),
    )


KEYS = (
    pltpu.VMEM((U * T // KB, KB, D), BF16),
    pltpu.VMEM((U * T // KB, KB, D), BF16),
    pltpu.VMEM((U * T // KB, KB, D), F32),
    pltpu.VMEM((U, 8, 2 * T), F32),
    pltpu.VMEM((U, 8, 2 * T), F32),
    pltpu.VMEM((U, 8, T), F32),
)
SUM_Q = pltpu.VMEM((U, D, 2 * T), F32)
SUM_KV = pltpu.VMEM((U, 2 * T, D), F32)


def shape(*dims, dtype=BF16):
    return jax.ShapeDtypeStruct(dims, dtype)


def exchanged(message):
    return lax.all_to_all(message, ULY, 0, 0, tiled=True)


def moved(block, distance):
    count = lax.axis_size("blk")
    route = [(i, i + distance) for i in range(count) if 0 <= i + distance < count]
    return lax.ppermute(block, "blk", route)


def join_kernel(first_ref, second_ref, out_ref):
    out_ref[:, 0:KROWS, :] = first_ref[...]
    out_ref[:, KROWS:, :] = second_ref[:, 0 : 2 * T, :]


def in_hbm(x):
    return pltpu.with_memory_space_constraint(x, pltpu.HBM)


def stages(query, key, value, forward_out, out_grad, lse_parts, ids):
    ids = ids.reshape(1, T)
    message = call(pack_q_kernel, shape(U, QROWS, D), flops=1 << 20)(
        *map(in_hbm, (query, out_grad, forward_out, lse_parts.transpose(1, 2, 0), ids))
    )
    rows = exchanged(message)
    kv_msg = call(pack_kv_kernel, shape(U, KROWS, D), flops=1 << 20)(key, value, ids)
    prev_raw = moved(kv_msg, 1)
    later_rows = moved(rows, -1)
    both = call(join_kernel, shape(U, KROWS + 2 * T, D), flops=1 << 20)(prev_raw, kv_msg)
    keys = exchanged(both)
    tall, wide, half = shape(U, 2 * T, D, dtype=F32), shape(U, D, 2 * T, dtype=F32), shape(U, 2 * T, D)
    dq, dprev = call(prev_kernel, (wide, tall), KEYS, flops=4 << 30)(rows, keys)
    dq_msg, dkv_msg = call(far_kernel, (half, half), (SUM_Q, SUM_KV) + KEYS, flops=1 << 30)(later_rows, keys, dprev)
    dkv_back = moved(dkv_msg, -1)
    dq_back = moved(dq_msg, 1)
    dq, down = call(own_kernel, (tall, tall), (SUM_Q,) + KEYS, flops=4 << 30)(rows, keys, dq)
    total = call(total_kernel, shape(U, 4 * T, D), flops=1 << 20)(dq, dq_back, down, dkv_back)
    return call(unpack_kernel, (shape(T, 2 * U * D), shape(T, U * D), shape(T, U * D)), flops=1 << 20)(exchanged(total))


def solution(mesh):
    torus = Mesh(mesh.devices.reshape(4, 2, mesh.shape["blk"]), ("uly_0", "uly_1", "blk"))
    flat, cube, line = P(BLK_ULY, None), P(BLK_ULY, None, None), P(BLK_ULY)
    return jax.shard_map(
        stages,
        mesh=torus,
        in_specs=(flat, flat, flat, flat, flat, cube, line),
        out_specs=(flat, flat, flat),
        check_vma=False,
    )
```
